32 devices in a mesh: fsdp: 8 (over z, x), rep: 4 (over y, core).
Axes of the slice: x: 2, y: 2, z: 4, core: 2. Of those that a mesh axis runs over, the one named last changes fastest.
Arguments:
- activations: bfloat16 [2, 8, 512, 768], P(None, 'fsdp', 'rep'), may hold values from -6 to 6
- spatial: bfloat16 [2, 8, 512, 768], P(None, 'fsdp', 'rep'), may hold values from -6 to 6
- buckets: int32 [2, 3, 8, 512], P(None, None, 'fsdp'), may hold values from 0 to 15
- page_valid: int32 [8], P('fsdp'), may hold values 0 or 1
- qkv_w: bfloat16 [1, 2, 3, 768, 768], P(None, None, None, 'fsdp'), may hold values from -0.21875 to 0.21875
- out_w: bfloat16 [1, 2, 768, 768], P(None, None, 'fsdp'), may hold values from -1.5 to 1.5
- up_w: bfloat16 [1, 2, 768, 3072], P(None, None, 'fsdp'), may hold values from -0.21875 to 0.21875
- down_w: bfloat16 [1, 2, 3072, 768], P(None, None, 'fsdp'), may hold values from -0.109375 to 0.109375
- spatial_w: bfloat16 [2, 768, 768], P(None, 'fsdp'), may hold values from -0.21875 to 0.21875
- tables: bfloat16 [1, 2, 3, 12, 31], replicated, may hold values from -3 to 3
- norm_gains: bfloat16 [1, 2, 2, 768], P(None, None, None, 'fsdp'), may hold values from 0.25 to 1.75
- biases: bfloat16 [1, 2, 2, 768], P(None, None, None, 'fsdp'), may hold values from -1 to 1
- cotangent: bfloat16 [2, 8, 512, 768], P(None, 'fsdp', 'rep'), may hold values from -6 to 6
Outputs:
- layer_out: bfloat16 [2, 8, 512, 768], P(None, 'fsdp', 'rep')
- in_grad: float32 [2, 8, 512, 768], P(None, 'fsdp', 'rep')
- qkv_grad: float32 [1, 2, 3, 768, 768], P(None, None, None, 'fsdp')
- out_grad: float32 [1, 2, 768, 768], P(None, None, 'fsdp')
- up_grad: float32 [1, 2, 768, 3072], P(None, None, 'fsdp')
- down_grad: float32 [1, 2, 3072, 768], P(None, None, 'fsdp')
- spatial_grad: float32 [2, 768, 768], P(None, 'fsdp')
- table_grad: float32 [1, 2, 3, 12, 31], replicated
- gain_grad: float32 [1, 2, 2, 768], P(None, None, None, 'fsdp')
- bias_grad: float32 [1, 2, 2, 768], P(None, None, None, 'fsdp')
The draws below stay inside these ranges and needn't reach their ends.
Inputs may be any that keep to these rules, and one draw needn't show every extreme that they name: `buckets`: the bias of a pair of tokens is looked up by the difference of their values. `page_valid`: page slots with 0 hold padding and pass their input through.
All inputs are finite; a program needn't handle non-finite values. No bound on the sum of `page_valid` on one device may be relied on, other than what follows from the above.
Results may differ from the reference program's by a relative error of at most 0.018.
Values may be sent and summed in bfloat16 or wider, within the bound.
A program may use at most 256 MiB of HBM per device.

```python
from functools import partial
import jax
import jax.numpy as jnp
from jax import lax

D = 768
STREAM_HEADS = 12
HEAD_WIDTH = 64
FF = 3072
PAGE_TOKENS = 512
BINS = 16
LAYERS = 1
PAGES = 8


def touch_ends(entries, rng, smallest, largest):
    shape = entries.shape
    place = [jax.random.randint(jax.random.fold_in(rng, axis), (), 0, shape[axis]) for axis in range(len(shape))]
    entries = entries.at[tuple(place)].set(smallest)
    longest = shape.index(max(shape))
    place[longest] = (place[longest] + 1) % shape[longest]
    return entries.at[tuple(place)].set(largest)


def raised(result, rng, source, target, blocks, factor):
    owner, partner = [(jnp.arange(result.shape[axis_at]) // (result.shape[axis_at] // blocks)).reshape([-1 if axis == axis_at else 1 for axis in range(result.ndim)]) for axis_at in (source, target)]
    chosen = jax.random.permutation(rng, blocks)[partner]
    strong = (owner == chosen) | (owner == (partner + blocks // 2) % blocks)
    return jnp.where(strong, factor * result, result)


def levels(own_key, extent, split, smallest, top_value):
    gain, own = 1.0, jax.random.fold_in(own_key, 6)
    for axis_at, parts in split:
        steps = jnp.exp(jax.random.uniform(jax.random.fold_in(own, axis_at), (parts,), jnp.float32, smallest / len(split), top_value / len(split)))
        gain = gain * jnp.repeat(steps, extent[axis_at] // parts).reshape([-1 if axis == axis_at else 1 for axis in range(len(extent))])
    return gain


def gaussian(own_key, extent, scale, bound, cuts=(), kind=jnp.bfloat16):
    entries = jax.random.normal(own_key, extent, jnp.float32) * scale
    if len(cuts) > 0:
        entries = levels(own_key, extent, cuts, -0.22, 0.18) * entries
    return jnp.clip(entries, min=-bound, max=bound).astype(kind)


def bell_draw_with(rng, dims, scale, reach, cuts, heavy, kind=jnp.bfloat16):
    drawn = scale * jax.random.normal(rng, dims, jnp.float32)
    if cuts:
        drawn = drawn * levels(rng, dims, cuts, -0.22, 0.18)
    return jnp.clip(raised(drawn, jax.random.fold_in(rng, 3), *heavy), -reach, reach).astype(kind)


def setup_inputs(seed: int = 0) -> dict:
    arg_keys = jax.random.split(jax.random.key(seed), 14)
    activations = gaussian(arg_keys[0], (2, PAGES, PAGE_TOKENS, D), 1.0, 6.0, ((1, 8), (2, 4)))
    spatial = gaussian(arg_keys[1], (2, PAGES, PAGE_TOKENS, D), 1.0, 6.0, ((1, 8), (2, 4)))
    buckets = touch_ends(jax.random.randint(arg_keys[2], (2, 3, PAGES, PAGE_TOKENS), 0, BINS), jax.random.fold_in(arg_keys[2], 1), 0, BINS - 1).astype(jnp.int32)
    page_valid = touch_ends((jax.random.randint(arg_keys[3], (PAGES,), 0, 5) < 3).astype(jnp.int32), jax.random.fold_in(arg_keys[3], 1), 0, 1)
    qkv_w = gaussian(arg_keys[4], (LAYERS, 2, 3, D, D), D ** -0.5, 0.21875, ((3, 8),))
    out_w = gaussian(arg_keys[5], (LAYERS, 2, D, D), (D // 48) ** -0.5, 1.5, ((2, 8),))
    up_w = gaussian(arg_keys[6], (LAYERS, 2, D, FF), D ** -0.5, 0.21875, ((2, 8),))
    down_w = gaussian(arg_keys[7], (LAYERS, 2, FF, D), FF ** -0.5, 0.109375, ((2, 8),))
    spatial_w = gaussian(arg_keys[8], (2, D, D), D ** -0.5, 0.21875, ((1, 8),))
    tables = gaussian(arg_keys[9], (LAYERS, 2, 3, STREAM_HEADS, 2 * BINS - 1), 0.5, 3.0)
    norm_gains = jnp.clip(1.0 + 0.15 * jax.random.normal(arg_keys[10], (LAYERS, 2, 2, D), jnp.float32), 0.25, 1.75).astype(jnp.bfloat16)
    biases = gaussian(arg_keys[11], (LAYERS, 2, 2, D), 0.2, 1.0, ((3, 8),))
    cotangent = bell_draw_with(arg_keys[12], (2, PAGES, PAGE_TOKENS, D), 1.0, 6.0, ((1, 8), (2, 4)), (1, 3, 8, 2.0))
    return dict(activations=activations, spatial=spatial, buckets=buckets, page_valid=page_valid, qkv_w=qkv_w, out_w=out_w, up_w=up_w, down_w=down_w, spatial_w=spatial_w, tables=tables, norm_gains=norm_gains, biases=biases, cotangent=cotangent)


HIGHEST = lax.Precision.HIGHEST
EPSILON = 1e-05

@jax.custom_vjp
def low(v):
    return lax.optimization_barrier(v.astype(jnp.bfloat16)).astype(jnp.float32)

@jax.custom_vjp
def low_back(v):
    return v

def low_keep(v):
    return (low(v), None)

def low_pass(kept, grad):
    return (grad,)

def back_keep(v):
    return (v, None)

def back_low(kept, grad):
    return (low(grad),)
low.defvjp(low_keep, low_pass)
low_back.defvjp(back_keep, back_low)

def matrix_product(form, left, right):
    return jnp.einsum(form, left, right, precision=HIGHEST)

def layer_norm(residual, gain_row, bias_row):
    centre = residual - lax.optimization_barrier(jnp.mean(residual, axis=-1, keepdims=True))
    spread = lax.optimization_barrier(jnp.mean(centre * centre, axis=-1, keepdims=True))
    return centre * lax.rsqrt(spread + EPSILON) * gain_row + bias_row

def shift_table():
    span = 2 * BINS - 1
    left = lax.broadcasted_iota(jnp.int32, (BINS, BINS, span), 0)
    right = lax.broadcasted_iota(jnp.int32, (BINS, BINS, span), 1)
    slot = lax.broadcasted_iota(jnp.int32, (BINS, BINS, span), 2)
    return (left - right + BINS - 1 == slot).astype(jnp.float32)

def page_forward(params, page_acts, page_spatial, page_buckets, page_flag):
    qkv_w, out_w, up_w, down_w, spatial_w, tables, norm_gains, biases = params
    attention_scale = HEAD_WIDTH ** (-0.5)
    one_hot = (page_buckets[..., None] == jnp.arange(BINS, dtype=jnp.int32)).astype(jnp.float32)
    one_hot = jnp.transpose(one_hot, (0, 2, 1, 3))
    key_bucket_rows = one_hot.reshape(2, PAGE_TOKENS, 3 * BINS)
    offsets = shift_table()
    layout_query = low_back(low(matrix_product('sid,de->sie', page_spatial, spatial_w[0])))
    layout_key = low_back(low(matrix_product('sid,de->sie', page_spatial, spatial_w[1])))
    spatial_query_heads = layout_query.reshape(2, PAGE_TOKENS, STREAM_HEADS, HEAD_WIDTH)
    spatial_key_heads = layout_key.reshape(2, PAGE_TOKENS, STREAM_HEADS, HEAD_WIDTH)
    current = page_acts
    for layer_idx in range(LAYERS):
        inputs = low(current)
        projected = low_back(low(matrix_product('sid,sjde->sjie', inputs, qkv_w[layer_idx])))
        query_matrix = projected[:, 0].reshape(2, PAGE_TOKENS, STREAM_HEADS, HEAD_WIDTH)
        keys = projected[:, 1].reshape(2, PAGE_TOKENS, STREAM_HEADS, HEAD_WIDTH)
        values = projected[:, 2].reshape(2, PAGE_TOKENS, STREAM_HEADS, HEAD_WIDTH)
        bias_mats = matrix_product('skhr,uvr->skhuv', tables[layer_idx], offsets)
        token_features = matrix_product('siku,skhuv->sihkv', one_hot, bias_mats).reshape(2, PAGE_TOKENS, STREAM_HEADS, 3 * BINS)
        direct = matrix_product('uvnt,urnt->unvr', query_matrix, keys)
        layout_portion = matrix_product('uvnt,urnt->unvr', spatial_query_heads, spatial_key_heads)
        scores = attention_scale * (direct + layout_portion) + matrix_product('sihc,sjc->shij', token_features, key_bucket_rows)
        scores = low_back(scores)
        attn_probs = jax.nn.softmax(scores, axis=-1)
        mixed_out = low_back(low(matrix_product('shij,sjhd->sihd', low(attn_probs), values))).reshape(2, PAGE_TOKENS, D)
        branch = low_back(matrix_product('sid,sde->sie', mixed_out, out_w[layer_idx]))
        residual = current + (branch[0] + branch[1])[None]
        hidden = layer_norm(residual, norm_gains[layer_idx][:, 0][:, None, :], biases[layer_idx][:, 0][:, None, :])
        gate_pre = low_back(matrix_product('sid,sdf->sif', low(hidden), up_w[layer_idx]))
        active = low(jax.nn.gelu(gate_pre, approximate=True))
        ffn_out = low_back(matrix_product('sif,sfd->sid', active, down_w[layer_idx]))
        current = layer_norm(hidden + ffn_out, norm_gains[layer_idx][:, 1][:, None, :], biases[layer_idx][:, 1][:, None, :])
    return jnp.where(page_flag > 0, current, page_acts)

def reference(activations, spatial, buckets, page_valid, qkv_w, out_w, up_w, down_w, spatial_w, tables, norm_gains, biases, cotangent):
    params = (qkv_w.astype(jnp.float32), out_w.astype(jnp.float32), up_w.astype(jnp.float32), down_w.astype(jnp.float32), spatial_w.astype(jnp.float32), tables.astype(jnp.float32), norm_gains.astype(jnp.float32), biases.astype(jnp.float32))
    acts_float = activations.astype(jnp.float32)
    spatial_pages = jnp.moveaxis(spatial.astype(jnp.float32), 1, 0)
    bucket_pages = jnp.moveaxis(buckets, 2, 0)

    def forward_all(acts_in, weights):
        page_step = jax.checkpoint(partial(page_forward, weights))

        def scan_step(carried, page_in):
            return (carried, page_step(*page_in))
        _, page_outs = lax.scan(scan_step, None, (jnp.moveaxis(acts_in, 1, 0), spatial_pages, bucket_pages, page_valid))
        return jnp.moveaxis(page_outs, 0, 1)
    layer_out, pullback = jax.vjp(forward_all, acts_float, params)
    in_grad, weight_grads = pullback(cotangent.astype(jnp.float32))
    return (layer_out.astype(jnp.bfloat16), in_grad, weight_grads[0], weight_grads[1], weight_grads[2], weight_grads[3], weight_grads[4], weight_grads[5], weight_grads[6], weight_grads[7])
```

```python
from functools import partial

import jax
import jax.numpy as jnp
from jax import lax
from jax.experimental import pallas as pl
from jax.experimental.pallas import tpu as pltpu
from jax.sharding import PartitionSpec as P

EPSILON = 1e-05
HIGHEST = lax.Precision.HIGHEST
F32 = jnp.float32
BF16 = jnp.bfloat16
MESH = pl.DeviceIdType.MESH


def low(value):
    return value.astype(BF16)


def wide(value):
    return value.astype(F32)


def dot(left, right, left_axis=1, right_axis=0, precision=None):
    dims = (((left_axis,), (right_axis,)), ((), ()))
    return lax.dot_general(left, right, dims, precision=precision, preferred_element_type=F32)


def pick(array, index, axis=0):
    return lax.dynamic_index_in_dim(array, index, axis, keepdims=False)


def core_swap(value):
    return lax.ppermute(value, "rep", [(0, 1), (1, 0), (2, 3), (3, 2)])


def y_swap(value):
    return lax.ppermute(value, "rep", [(0, 2), (2, 0), (1, 3), (3, 1)])


def ordered(flag, first, second, axis):
    return jnp.where(
        flag == 0,
        jnp.stack([first, second], axis),
        jnp.stack([second, first], axis),
    )


def places(fsdp):
    f = lax.axis_index("fsdp")
    r = lax.axis_index("rep")
    depth = fsdp // 2
    z, x = f // 2, f % 2
    up = ((z + 1) % depth) * 2
    down = ((z + depth - 1) % depth) * 2
    far = ((z + 2) % depth) * 2
    y, c = r // 2, r % 2
    return dict(
        f=f,
        r=r,
        y=y,
        c=c,
        other=z * 2 + 1 - x,
        up=up + x,
        up_other=up + 1 - x,
        down=down + x,
        down_other=down + 1 - x,
        far=far + x,
        far_other=far + 1 - x,
        r_y=(1 - y) * 2 + c,
        r_c=y * 2 + 1 - c,
    )


def greet(at):
    barrier = pltpu.get_barrier_semaphore()
    partners = (
        (at["other"], at["r"]),
        (at["up"], at["r"]),
        (at["down"], at["r"]),
        (at["f"], at["r_y"]),
        (at["f"], at["r_c"]),
    )
    for partner in partners:
        pl.semaphore_signal(barrier, inc=1, device_id=partner, device_id_type=MESH)
    pl.semaphore_wait(barrier, len(partners))


class Sender:
    def __init__(self, at, send, recv):
        self.at, self.send, self.recv = at, send, recv
        self.copies = []

    def __call__(self, source, target, where):
        at = self.at
        device = {
            "x": (at["other"], at["r"]),
            "up": (at["up"], at["r"]),
            "down": (at["down"], at["r"]),
            "y": (at["f"], at["r_y"]),
            "c": (at["f"], at["r_c"]),
        }[where]
        k = len(self.copies)
        copy = pltpu.make_async_remote_copy(
            src_ref=source,
            dst_ref=target,
            send_sem=self.send.at[k],
            recv_sem=self.recv.at[k],
            device_id=device,
            device_id_type=MESH,
        )
        copy.start()
        self.copies.append([copy, False])
        return self.copies[-1]

    def arrived(self, *entries):
        for entry in entries:
            if not entry[1]:
                entry[0].wait_recv()
                entry[1] = True

    def finish(self):
        self.arrived(*self.copies)
        for copy, _ in self.copies:
            copy.wait_send()


def gather_kernel(fsdp, count, *refs):
    shards, (acts, spatial, cot) = refs[:count], refs[count : count + 3]
    refs = refs[count + 3 :]
    full, (x_all, s_all, c_own) = refs[:count], refs[count : count + 3]
    send, recv, own = refs[count + 3 :]
    at = places(fsdp)
    greet(at)
    copy = Sender(at, send, recv)
    local = []

    def keep(source, target):
        local.append(pltpu.make_async_copy(source, target, own.at[len(local)]))
        local[-1].start()

    y, f = at["y"], at["f"]
    first = []
    swaps = []
    for source, target in ((acts, x_all), (spatial, s_all)):
        swaps.append((copy(source.at[1 - y, 0], target.at[1], "y"), target))
        copy(source.at[y, 0], target.at[2], "c")
        keep(source.at[y, 0], target.at[0])
    for shard, whole in zip(shards, full):
        half = shard.shape[0] // 2
        first.append(
            (
                copy(shard, whole.at[f], "x"),
                copy(shard, whole.at[f], "up"),
                copy(shard, whole.at[f], "down"),
            )
        )
        keep(shard, whole.at[f])
    copy(cot.at[1 - y, 0], c_own.at[1], "y")
    keep(cot.at[y, 0], c_own.at[0])
    for swap, target in swaps:
        copy.arrived(swap)
        copy(target.at[1], target.at[3], "c")
    second = []
    for (x_in, down_in, up_in), whole in zip(first, full):
        half = whole.shape[1] // 2
        copy.arrived(x_in)
        other = whole.at[at["other"]]
        copy(other, other, "up")
        copy(other, other, "down")
        copy.arrived(down_in, up_in)
        low_half = whole.at[at["down"], pl.ds(0, half)]
        high_half = whole.at[at["up"], pl.ds(half, half)]
        second.append((copy(low_half, low_half, "up"), copy(high_half, high_half, "down")))
    for (from_down, from_up), whole in zip(second, full):
        copy.arrived(from_down, from_up)
        far = whole.at[at["far"]]
        copy(far, far, "x")
    copy.finish()
    for entry in local:
        entry.wait()


def gather(fsdp, shards, acts, spatial, cot):
    count = len(shards)
    rows, width = acts.shape[2:]
    vmem, hbm = pl.BlockSpec(memory_space=pltpu.VMEM), pl.BlockSpec(memory_space=pl.ANY)
    copies = 7 + 8 * count
    shapes = [jax.ShapeDtypeStruct((fsdp,) + s.shape, BF16) for s in shards]
    shapes += [jax.ShapeDtypeStruct((n, rows, width), BF16) for n in (4, 4, 2)]
    return pl.pallas_call(
        partial(gather_kernel, fsdp, count),
        out_shape=shapes,
        in_specs=[vmem] * (count + 3),
        out_specs=[hbm] * (count + 3),
        scratch_shapes=[
            pltpu.SemaphoreType.DMA((copies,)),
            pltpu.SemaphoreType.DMA((copies,)),
            pltpu.SemaphoreType.DMA((count + 3,)),
        ],
        compiler_params=pltpu.CompilerParams(collective_id=0, has_side_effects=True),
        name="gather",
    )(*shards, acts, spatial, cot)


def gather_plain(shards, acts, spatial, cot, y):
    full = [lax.all_gather(s, "fsdp") for s in shards]

    def own_blocks(value):
        return jnp.stack([pick(value, y)[0], y_swap(pick(value, 1 - y)[0])])

    x_own, s_own, c_own = own_blocks(acts), own_blocks(spatial), own_blocks(cot)
    x_all = jnp.concatenate([x_own, core_swap(x_own)])
    s_all = jnp.concatenate([s_own, core_swap(s_own)])
    return full + [x_all, s_all, c_own]


def add_rows(out, terms, start, size):
    step = 16 if size % 16 == 0 else size

    def body(i, carry):
        at = pl.ds(pl.multiple_of(start + i * step, step), step)
        total = None
        for ref, offset in terms:
            part = wide(ref[pl.ds(pl.multiple_of(offset + i * step, step), step), :])
            total = part if total is None else total + part
        out[at, :] = total.astype(out.dtype)
        return carry

    lax.fori_loop(0, size // step, body, 0)


def reduce_kernel(fsdp, count, *refs):
    grads, results = refs[:count], refs[count : 2 * count]
    refs = refs[2 * count :]
    buffers = [refs[10 * q : 10 * q + 10] for q in range(count)]
    send, recv, own = refs[10 * count :]
    at = places(fsdp)
    greet(at)
    copy = Sender(at, send, recv)
    state = [dict() for _ in range(count)]
    local = []

    def begin(q):
        g = grads[q]
        x_in, q_down, q_up, from_down, from_up, x_last = buffers[q][:6]
        half = g.shape[1] // 2
        lo, hi = pl.ds(0, half), pl.ds(half, half)
        s = state[q]
        s["x"] = copy(g.at[at["far_other"]], x_in, "x")
        s["down"] = [
            copy(g.at[at["up_other"]], from_down.at[1], "up"),
            copy(g.at[at["up"], hi], from_down.at[0, hi], "up"),
        ]
        s["up"] = [
            copy(g.at[at["down_other"]], from_up.at[1], "down"),
            copy(g.at[at["down"], lo], from_up.at[0, lo], "down"),
        ]

    def far_sum(q):
        g = grads[q]
        x_in, q_down, q_up = buffers[q][:3]
        total = buffers[q][6]
        rows = g.shape[1]
        half = rows // 2
        s = state[q]
        copy.arrived(s["x"])
        add_rows(total, ((g.at[at["far"]], 0), (x_in, 0)), 0, rows)
        s["q_down"] = copy(total.at[pl.ds(0, half)], q_down, "up")
        s["q_up"] = copy(total.at[pl.ds(half, half)], q_up, "down")

    def near_sum(q):
        g = grads[q]
        _, q_down, q_up, from_down, from_up, _ = buffers[q][:6]
        total = buffers[q][7]
        half = g.shape[1] // 2
        lo, hi = pl.ds(0, half), pl.ds(half, half)
        s = state[q]
        copy.arrived(s["q_down"])
        add_rows(total, ((g.at[at["up"]], 0), (q_down, 0)), 0, half)
        s["down"].append(copy(total.at[lo], from_down.at[0, lo], "up"))
        copy.arrived(s["q_up"])
        add_rows(total, ((g.at[at["down"]], half), (q_up, 0)), half, half)
        s["up"].append(copy(total.at[hi], from_up.at[0, hi], "down"))

    def column_sum(q):
        g = grads[q]
        from_down, from_up, x_last = buffers[q][3:6]
        mine, theirs = buffers[q][8], buffers[q][6]
        rows = g.shape[1]
        s = state[q]
        copy.arrived(*s["down"], *s["up"])
        s["far_sent"] = (s["q_down"], s["q_up"])
        for entry in s["far_sent"]:
            entry[0].wait_send()
            entry.append(True)
        add_rows(theirs, ((g.at[at["other"]], 0), (from_down.at[1], 0), (from_up.at[1], 0)), 0, rows)
        s["x_last"] = copy(theirs, x_last, "x")
        add_rows(mine, ((g.at[at["f"]], 0), (from_down.at[0], 0), (from_up.at[0], 0)), 0, rows)

    def own_sum(q):
        mine, x_last, total = buffers[q][8], buffers[q][5], buffers[q][9]
        rows = total.shape[0]
        res = results[q]
        s = state[q]
        copy.arrived(s["x_last"])
        add_rows(total, ((mine, 0), (x_last, 0)), 0, rows)
        s["y"] = copy(total, res.at[2], "y")
        copy(total, res.at[1], "c")
        local.append(pltpu.make_async_copy(total, res.at[0], own.at[q]))
        local[-1].start()

    def hand_on(q):
        s = state[q]
        copy.arrived(s["y"])
        copy(results[q].at[2], results[q].at[3], "c")

    stages = (begin, far_sum, near_sum, column_sum, own_sum, hand_on)
    delays = (0, 1, 2, 3, 4, 5)
    for step in range(count + delays[-1]):
        for stage, delay in reversed(tuple(zip(stages, delays))):
            if stage is begin:
                continue
            if 0 <= step - delay < count:
                stage(step - delay)
        if step == 0:
            begin(0)
            if count > 1:
                begin(1)
        elif step + 1 < count:
            begin(step + 1)
    copy.arrived(*copy.copies)
    for entry in copy.copies:
        if len(entry) == 2:
            entry[0].wait_send()
    for entry in local:
        entry.wait()


def reduce(fsdp, grads):
    count = len(grads)
    vmem, hbm = pl.BlockSpec(memory_space=pltpu.VMEM), pl.BlockSpec(memory_space=pl.ANY)
    scratch = []
    for g in grads:
        _, rows, cols = g.shape
        scratch += [
            pltpu.VMEM((rows, cols), BF16),
            pltpu.VMEM((rows // 2, cols), BF16),
            pltpu.VMEM((rows // 2, cols), BF16),
            pltpu.VMEM((2, rows, cols), BF16),
            pltpu.VMEM((2, rows, cols), BF16),
            pltpu.VMEM((rows, cols), BF16),
            pltpu.VMEM((rows, cols), BF16),
            pltpu.VMEM((rows, cols), BF16),
            pltpu.VMEM((rows, cols), F32),
            pltpu.VMEM((rows, cols), BF16),
        ]
    copies = 13 * count
    return pl.pallas_call(
        partial(reduce_kernel, fsdp, count),
        out_shape=[jax.ShapeDtypeStruct((4,) + g.shape[1:], BF16) for g in grads],
        in_specs=[vmem] * count,
        out_specs=[hbm] * count,
        scratch_shapes=scratch
        + [
            pltpu.SemaphoreType.DMA((copies,)),
            pltpu.SemaphoreType.DMA((copies,)),
            pltpu.SemaphoreType.DMA((count,)),
        ],
        compiler_params=pltpu.CompilerParams(
            collective_id=1, has_side_effects=True, vmem_limit_bytes=48 << 20
        ),
        name="reduce",
    )(*grads)


def reduce_plain(grads):
    results = []
    for g in grads:
        total = lax.psum_scatter(g, "fsdp", scatter_dimension=0, tiled=True)[0]
        far = y_swap(total)
        results.append(jnp.stack([total, core_swap(total), far, core_swap(far)]))
    return results


def pair_mask(lanes, head_width, t):
    lane = lax.broadcasted_iota(jnp.int32, (1, lanes), 1)
    return ((lane % 128) // head_width == t).astype(BF16)


def attention_kernel(head_width, scale, q, k, v, sq, sk, hot_ref, bias, mixed, probs):
    keys = jnp.concatenate([k[...], sk[...]], axis=1)
    queries = jnp.concatenate([q[...], sq[...]], axis=1) * scale
    hot = hot_ref[...]
    value = v[...]
    parts = []
    for t in range(128 // head_width):
        masked = queries * pair_mask(256, head_width, t)
        feature = low(dot(hot, bias[t]))
        scores = dot(keys, masked, 1, 1) + dot(hot, feature, 1, 1)
        top = jnp.max(scores, axis=0, keepdims=True)
        raised = jnp.exp(scores - top)
        prob = low(raised * (1.0 / jnp.sum(raised, axis=0, keepdims=True)))
        probs[t] = prob
        both = dot(value, prob, 0, 0)
        parts.append(both[t * head_width : (t + 1) * head_width])
    mixed[...] = low(jnp.transpose(jnp.concatenate(parts, axis=0)))


def attention(qkv, spk, hot, bias, head_width):
    tokens = qkv.shape[0]
    heads = bias.shape[0]
    per = 128 // head_width
    groups = heads // per
    full = lambda g: (0, 0)
    at = lambda j: pl.BlockSpec((tokens, 128), lambda g: (0, j * groups + g))
    return pl.pallas_call(
        partial(attention_kernel, head_width, head_width**-0.5),
        grid=(groups,),
        out_shape=(
            jax.ShapeDtypeStruct((tokens, heads * head_width), BF16),
            jax.ShapeDtypeStruct((heads, tokens, tokens), BF16),
        ),
        in_specs=[
            at(0),
            at(1),
            at(2),
            at(0),
            at(1),
            pl.BlockSpec(hot.shape, full),
            pl.BlockSpec((per,) + bias.shape[1:], lambda g: (g, 0, 0)),
        ],
        out_specs=[
            pl.BlockSpec((tokens, 128), lambda g: (0, g)),
            pl.BlockSpec((per, tokens, tokens), lambda g: (g, 0, 0)),
        ],
        compiler_params=pltpu.CompilerParams(vmem_limit_bytes=48 << 20),
        name="attention",
    )(qkv, qkv, qkv, spk, spk, hot, bias)


def attention_back_kernel(
    head_width, scale, groups, q, k, v, sq, sk, hot_ref, probs, mixed_grad, grad, sgrad, corner
):
    g = pl.program_id(0)
    keys = jnp.concatenate([k[...], sk[...]], axis=1)
    queries = jnp.concatenate([q[...], sq[...]], axis=1) * scale
    hot = hot_ref[...]
    value = v[...]
    outer = mixed_grad[...]
    key_total = value_total = None
    query_rows = [[], []]
    for t in range(128 // head_width):
        outer_t = outer * pair_mask(128, head_width, t)
        prob = probs[t]
        prob_wide = wide(prob)
        prob_grad = dot(value, outer_t, 1, 1)
        delta = jnp.sum(prob_wide * prob_grad, axis=0, keepdims=True)
        score_grad = low(prob_wide * (prob_grad - delta))
        value_part = dot(prob, outer_t)
        key_part = dot(score_grad, queries * pair_mask(256, head_width, t))
        key_total = key_part if t == 0 else key_total + key_part
        value_total = value_part if t == 0 else value_total + value_part
        query_t = dot(keys, score_grad, 0, 0)
        for half in range(2):
            start = half * 128 + t * head_width
            query_rows[half].append(query_t[start : start + head_width])
        feature_grad = dot(hot, score_grad, 0, 0)
        high = low(feature_grad)
        rest = low(feature_grad - wide(high))
        corner[t] = dot(high, hot) + dot(rest, hot)
    query_total = jnp.transpose(jnp.concatenate(query_rows[0] + query_rows[1], axis=0)) * scale

    def place(j):
        return pl.ds(pl.multiple_of(j * groups * 128 + g * 128, 128), 128)

    grad[:, place(0)] = low(query_total[:, :128])
    grad[:, place(1)] = low(key_total[:, :128])
    grad[:, place(2)] = low(value_total)
    sgrad[:, place(0)] = low(query_total[:, 128:])
    sgrad[:, place(1)] = low(key_total[:, 128:])


def attention_back(qkv, spk, hot, probs, mixed_grad, head_width):
    tokens = qkv.shape[0]
    heads = probs.shape[0]
    per = 128 // head_width
    groups = heads // per
    wide_hot = hot.shape[1]
    full = lambda g: (0, 0)
    at = lambda j: pl.BlockSpec((tokens, 128), lambda g: (0, j * groups + g))
    return pl.pallas_call(
        partial(attention_back_kernel, head_width, head_width**-0.5, groups),
        grid=(groups,),
        out_shape=(
            jax.ShapeDtypeStruct(qkv.shape, BF16),
            jax.ShapeDtypeStruct(spk.shape, BF16),
            jax.ShapeDtypeStruct((heads, wide_hot, wide_hot), F32),
        ),
        in_specs=[
            at(0),
            at(1),
            at(2),
            at(0),
            at(1),
            pl.BlockSpec(hot.shape, full),
            pl.BlockSpec((per, tokens, tokens), lambda g: (g, 0, 0)),
            at(0),
        ],
        out_specs=[
            pl.BlockSpec(qkv.shape, full),
            pl.BlockSpec(spk.shape, full),
            pl.BlockSpec((per, wide_hot, wide_hot), lambda g: (g, 0, 0)),
        ],
        compiler_params=pltpu.CompilerParams(vmem_limit_bytes=48 << 20),
        name="attention_back",
    )(qkv, qkv, qkv, spk, spk, hot, probs, mixed_grad)


def norm_forward(residual, gain_row, bias_row):
    centre = residual - jnp.mean(residual, axis=-1, keepdims=True)
    inv_std = lax.rsqrt(jnp.mean(centre * centre, axis=-1, keepdims=True) + EPSILON)
    normed = centre * inv_std
    return normed * gain_row + bias_row, normed, inv_std


def norm_backward(grad_out, normed, inv_std, gain_row):
    scaled = grad_out * gain_row
    mean_one = jnp.mean(scaled, axis=-1, keepdims=True)
    mean_two = jnp.mean(scaled * normed, axis=-1, keepdims=True)
    grad_in = inv_std * (scaled - mean_one - normed * mean_two)
    return grad_in, jnp.sum(grad_out * normed, axis=0), jnp.sum(grad_out, axis=0)


def per_device(
    fsdp,
    activations,
    spatial,
    buckets,
    page_valid,
    qkv_w,
    out_w,
    up_w,
    down_w,
    spatial_w,
    tables,
    norm_gains,
    biases,
    cotangent,
):
    rows, width = activations.shape[2:]
    tokens = buckets.shape[3]
    heads = tables.shape[3]
    head_width = width // heads
    bins = (tables.shape[4] + 1) // 2
    own_heads = heads // 2
    own_width = width // 2
    shard_rows = qkv_w.shape[3]
    ff = up_w.shape[3]
    unit = ff // fsdp // 2
    own_ff = ff // 2
    rep = lax.axis_index("rep")
    y, c = rep // 2, rep % 2

    def columns(array, axis):
        return lax.dynamic_slice_in_dim(array, c * own_width, own_width, axis)

    qkv_part = jnp.transpose(columns(pick(qkv_w[0], y), 2), (1, 0, 2)).reshape(shard_rows, -1)
    spatial_part = jnp.transpose(columns(spatial_w, 2), (1, 0, 2)).reshape(shard_rows, -1)
    params = jnp.concatenate([pick(norm_gains[0], y), pick(biases[0], y)]).T
    out_part = jnp.concatenate(
        [columns(pick(out_w[0], y), 1), jnp.pad(params, ((0, 0), (0, 124)))], axis=1
    )
    up_part = pick(pick(up_w[0], y).reshape(shard_rows, fsdp, 2, unit), c, 2)
    up_part = up_part.reshape(shard_rows, own_ff)
    down_part = pick(pick(down_w[0], y).reshape(2, unit, width), c)
    shards = (qkv_part, spatial_part, out_part, up_part, down_part)
    if fsdp == 8:
        gathered = gather(fsdp, shards, activations, spatial, cotangent)
    else:
        gathered = gather_plain(shards, activations, spatial, cotangent, y)
    w_qkv, w_spatial, w_out, w_up, w_down = [g.reshape(-1, g.shape[2]) for g in gathered[:5]]
    x_all, s_all, cot = [g.reshape(-1, width) for g in gathered[5:]]
    own = tokens // 2
    block = rows

    norms = wide(w_out[:, own_width : own_width + 4]).T
    gain_one, gain_two, bias_one, bias_two = [norms[i][None] for i in range(4)]
    mine = lax.dynamic_slice(w_out, (c * own_width, 0), (own_width, own_width))
    give = lax.dynamic_slice(w_out, ((1 - c) * own_width, 0), (own_width, own_width))
    w_own = ordered(c, mine, core_swap(give), 1).reshape(own_width, width)

    page_buckets = pick(buckets, y)[:, 0].reshape(3, 4, block)
    order = [rep, y_of(rep), c_of(rep), y_of(c_of(rep))]
    page_buckets = jnp.concatenate([pick(page_buckets, i, 1) for i in order], axis=1)
    hot = (page_buckets[..., None] == jnp.arange(bins, dtype=jnp.int32)).astype(BF16)
    hot = jnp.transpose(hot, (1, 0, 2)).reshape(tokens, 3 * bins)
    left = lax.broadcasted_iota(jnp.int32, (bins, bins, 2 * bins - 1), 0)
    right = lax.broadcasted_iota(jnp.int32, (bins, bins, 2 * bins - 1), 1)
    slot = lax.broadcasted_iota(jnp.int32, (bins, bins, 2 * bins - 1), 2)
    offsets = (left - right + bins - 1 == slot).astype(F32)
    own_tables = lax.dynamic_slice_in_dim(pick(tables[0], y), c * own_heads, own_heads, 1)
    matrices = jnp.einsum("khr,uvr->hkuv", wide(own_tables), offsets, precision=HIGHEST)
    bias = jnp.einsum("hkuv,kq->hkuqv", matrices, jnp.eye(3, dtype=F32), precision=HIGHEST)
    bias = low(bias.reshape(own_heads, 3 * bins, 3 * bins))

    valid = page_valid[0] > 0
    x_own = wide(x_all[:own])
    qkv = low(dot(x_all, w_qkv))
    spk = low(dot(s_all, w_spatial))
    mixed, probs = attention(qkv, spk, hot, bias, head_width)

    def core_sum(partial_sum):
        return partial_sum[:own] + wide(core_swap(low(partial_sum[own:])))

    def both_cores(value):
        return jnp.concatenate([value, core_swap(value)])

    def other_stream(value):
        sent = low(value)
        return wide(y_swap(jnp.concatenate([sent[block:], sent[:block]])))

    branch = core_sum(dot(mixed, w_own))
    residual = x_own + (branch + other_stream(branch))
    hidden, normed_one, inv_one = norm_forward(residual, gain_one, bias_one)
    hidden_all = both_cores(low(hidden))
    gate = dot(hidden_all, w_up)
    active = low(jax.nn.gelu(gate, approximate=True))
    ffn = core_sum(dot(active, w_down))
    result, normed_two, inv_two = norm_forward(hidden + ffn, gain_two, bias_two)
    layer_out = low(jnp.where(valid, result, x_own))
    layer_out = ordered(y, layer_out[:block], y_swap(layer_out[block:]), 0)[:, None]

    upstream = jnp.where(valid, wide(cot), 0.0)
    back_two, gain_two_grad, bias_two_grad = norm_backward(upstream, normed_two, inv_two, gain_two)
    ffn_grad = both_cores(low(back_two))
    down_grad = low(dot(active, ffn_grad, 0, 0))
    active_grad = dot(ffn_grad, w_down, 1, 1)
    pull = jax.vjp(partial(jax.nn.gelu, approximate=True), gate)[1]
    gate_grad = low(pull(active_grad)[0])
    up_grad = low(dot(hidden_all, gate_grad, 0, 0))
    hidden_grad = back_two + core_sum(dot(gate_grad, w_up, 1, 1))
    back_one, gain_one_grad, bias_one_grad = norm_backward(
        hidden_grad, normed_one, inv_one, gain_one
    )
    branch_grad = both_cores(low(back_one + other_stream(back_one)))
    mixed_grad = low(dot(branch_grad, w_own, 1, 1))
    out_own = low(dot(mixed, branch_grad, 0, 0))
    out_kept = columns(out_own, 1)
    out_given = lax.dynamic_slice_in_dim(out_own, (1 - c) * own_width, own_width, 1)
    out_grad = ordered(c, out_kept, core_swap(out_given), 0).reshape(width, own_width)
    norm_grads = jnp.stack([gain_one_grad, gain_two_grad, bias_one_grad, bias_two_grad], 1)
    out_grad = jnp.concatenate([out_grad, jnp.pad(low(norm_grads), ((0, 0), (0, 124)))], axis=1)
    grad, sgrad, corner = attention_back(qkv, spk, hot, probs, mixed_grad, head_width)
    qkv_grad = low(dot(x_all, grad, 0, 0))
    spatial_grad = low(dot(s_all, sgrad, 0, 0))
    in_own = back_one + core_sum(dot(grad, w_qkv, 1, 1))
    in_own = jnp.where(valid, in_own, wide(cot))
    in_far = wide(y_swap(low(in_own[block:])))
    in_grad = ordered(y, in_own[:block], in_far, 0)[:, None]

    corner = corner.reshape(own_heads, 3, bins, 3, bins)
    corner = jnp.stack([corner[:, k, :, k, :] for k in range(3)])
    table = jnp.einsum("khvu,uvr->khr", corner, offsets, precision=HIGHEST)
    table = lax.all_gather(table, ("fsdp", "rep"))
    table = table.reshape((fsdp, 2, 2) + table.shape[1:]).sum(axis=0)
    table_grad = jnp.transpose(table, (0, 2, 1, 3, 4)).reshape(tables.shape)

    grads = [
        g.reshape(fsdp, -1, g.shape[1])
        for g in (down_grad, up_grad, qkv_grad, spatial_grad, out_grad)
    ]
    reduced = reduce(fsdp, grads) if fsdp == 8 else reduce_plain(grads)
    down_r, up_r, qkv_r, spatial_r, out_r = [wide(r) for r in reduced]

    def whole(parts, axis):
        streams = [ordered(c, parts[2 * s], parts[2 * s + 1], axis) for s in range(2)]
        return ordered(y, streams[0], streams[1], 0)

    down_grad = whole(down_r, 0).reshape(down_w.shape)
    up_grad = whole(up_r.reshape(4, shard_rows, fsdp, unit), 2).reshape(up_w.shape)
    qkv_grad = whole(qkv_r.reshape(4, shard_rows, 3, own_width), 2)
    qkv_grad = jnp.transpose(qkv_grad.reshape(2, shard_rows, 3, width), (0, 2, 1, 3))[None]
    out_grad = whole(out_r[:, :, :own_width], 1).reshape(out_w.shape)
    spatial_sum = spatial_r[:2] + spatial_r[2:]
    spatial_sum = spatial_sum.reshape(2, shard_rows, 2, own_width)
    spatial_grad = ordered(c, spatial_sum[0], spatial_sum[1], 2).reshape(shard_rows, 2, width)
    spatial_grad = jnp.transpose(spatial_grad, (1, 0, 2))
    norm_sum = out_r[:, :, own_width : own_width + 4]
    norm_sum = jnp.transpose(norm_sum[0::2] + norm_sum[1::2], (0, 2, 1))
    norm_sum = ordered(y, norm_sum[0], norm_sum[1], 0)
    gain_grad, bias_grad = norm_sum[None, :, :2], norm_sum[None, :, 2:]
    return (
        layer_out,
        in_grad,
        qkv_grad,
        out_grad,
        up_grad,
        down_grad,
        spatial_grad,
        table_grad,
        gain_grad,
        bias_grad,
    )


def y_of(rep):
    return (rep + 2) % 4


def c_of(rep):
    return rep + 1 - 2 * (rep % 2)


def solution(mesh):
    weight = P(None, None, "fsdp", None)
    tokens = P(None, "fsdp", "rep", None)
    qkv = P(None, None, None, "fsdp", None)
    norm = P(None, None, None, "fsdp")
    return jax.shard_map(
        partial(per_device, mesh.shape["fsdp"]),
        mesh=mesh,
        in_specs=(
            tokens,
            tokens,
            weight,
            P("fsdp"),
            qkv,
            weight,
            weight,
            weight,
            P(None, "fsdp", None),
            P(),
            norm,
            norm,
            tokens,
        ),
        out_specs=(
            tokens,
            tokens,
            qkv,
            weight,
            weight,
            weight,
            P(None, "fsdp", None),
            P(),
            norm,
            norm,
        ),
        check_vma=False,
    )
```

```python
from functools import partial

import jax
import jax.numpy as jnp
from jax import lax
from jax.experimental import pallas as pl
from jax.experimental.pallas import tpu as pltpu
from jax.sharding import PartitionSpec as P

EPSILON = 1e-05
HIGHEST = lax.Precision.HIGHEST
F32 = jnp.float32
BF16 = jnp.bfloat16
MESH = pl.DeviceIdType.MESH


def low(value):
    return value.astype(BF16)


def wide(value):
    return value.astype(F32)


def dot(left, right, left_axis=1, right_axis=0, precision=None):
    dims = (((left_axis,), (right_axis,)), ((), ()))
    return lax.dot_general(left, right, dims, precision=precision, preferred_element_type=F32)


def pick(array, index, axis=0):
    return lax.dynamic_index_in_dim(array, index, axis, keepdims=False)


def core_swap(value):
    return lax.ppermute(value, "rep", [(0, 1), (1, 0), (2, 3), (3, 2)])


def y_swap(value):
    return lax.ppermute(value, "rep", [(0, 2), (2, 0), (1, 3), (3, 1)])


def ordered(flag, first, second, axis):
    return jnp.where(
        flag == 0,
        jnp.stack([first, second], axis),
        jnp.stack([second, first], axis),
    )


def places(fsdp):
    f = lax.axis_index("fsdp")
    r = lax.axis_index("rep")
    y, c = r // 2, r % 2
    return dict(
        f=f,
        r=r,
        y=y,
        c=c,
        z=f // 2,
        x=f % 2,
        depth=fsdp // 2,
        other=f + 1 - 2 * (f % 2),
        up=(f + 2) % fsdp,
        down=(f + fsdp - 2) % fsdp,
        r_y=(1 - y) * 2 + c,
        r_c=y * 2 + 1 - c,
    )


def greet(partners):
    barrier = pltpu.get_barrier_semaphore()
    for partner in partners:
        pl.semaphore_signal(barrier, inc=1, device_id=partner, device_id_type=MESH)
    pl.semaphore_wait(barrier, len(partners))


def when(condition, action):
    if condition is None:
        action()
    else:
        pl.when(condition)(action)


class Entry:
    def __init__(self, copy, sent, got):
        self.copy, self.sent, self.got = copy, sent, got
        self.seen = False

    def start(self):
        when(self.sent, self.copy.start)

    def arrived(self):
        if not self.seen:
            self.seen = True
            when(self.got, self.copy.wait_recv)


class Sender:
    def __init__(self, at, send, recv):
        self.send, self.recv = send, recv
        self.entries = []
        self.devices = {
            "x": (at["other"], at["r"]),
            "up": (at["up"], at["r"]),
            "down": (at["down"], at["r"]),
            "y": (at["f"], at["r_y"]),
            "c": (at["f"], at["r_c"]),
        }

    def make(self, source, target, where, sent=None, got=None):
        k = len(self.entries)
        copy = pltpu.make_async_remote_copy(
            src_ref=source,
            dst_ref=target,
            send_sem=self.send.at[k],
            recv_sem=self.recv.at[k],
            device_id=self.devices[where] if isinstance(where, str) else where,
            device_id_type=MESH,
        )
        self.entries.append(Entry(copy, sent, got))
        return self.entries[-1]

    def __call__(self, *given, **named):
        entry = self.make(*given, **named)
        entry.start()
        return entry

    def finish(self):
        for entry in self.entries:
            entry.arrived()
        for entry in self.entries:
            when(entry.sent, entry.copy.wait_send)


def gather_kernel(fsdp, sizes, *refs):
    qkv_w, out_w, down_w, spatial_w, up_part, params, acts, spatial, cot = refs[:9]
    full, (x_all, s_all, c_own) = refs[9:15], refs[15:18]
    send, recv, own = refs[18:]
    at = places(fsdp)
    y, c, f, z, x, depth = [at[k] for k in ("y", "c", "f", "z", "x", "depth")]
    copy = Sender(at, send, recv)
    greet(list(copy.devices.values()))
    half, unit = sizes
    columns = pl.ds(pl.multiple_of(c * half, 128), half)
    shards = (
        qkv_w.at[0, y, :, :, columns],
        spatial_w.at[:, :, columns],
        out_w.at[0, pl.ds(y, 1), :, columns],
        params,
        up_part,
        down_w.at[0, pl.ds(y, 1), pl.ds(pl.multiple_of(c * unit, 16), unit), :],
    )
    local = []

    def keep(source, target):
        local.append(pltpu.make_async_copy(source, target, own.at[len(local)]))
        local[-1].start()

    swaps = []
    for source, target in ((acts, x_all), (spatial, s_all)):
        swaps.append((copy(source.at[1 - y, 0], target.at[1], "y"), target))
        copy(source.at[y, 0], target.at[2], "c")
        keep(source.at[y, 0], target.at[0])
    rising, falling = [], []
    for shard, whole in zip(shards, full):
        copy(shard, whole.at[:, f], "x")
        rising.append(copy(shard, whole.at[:, f], "up", z < depth - 1, z > 0))
        falling.append(copy(shard, whole.at[:, f], "down", z > 0, z < depth - 1))
        keep(shard, whole.at[:, f])
    copy(cot.at[1 - y, 0], c_own.at[1], "y")
    keep(cot.at[y, 0], c_own.at[0])
    for swap, target in swaps:
        swap.arrived()
        copy(target.at[1], target.at[3], "c")
    for step in range(1, depth):
        for q, whole in enumerate(full):
            got = z >= step
            rising[q].arrived()
            piece = whole.at[:, (z - step) * 2 + x]
            copy(piece, piece, "x", got, got)
            if step + 1 < depth:
                go = (z >= step) & (z < depth - 1)
                rising[q] = copy(piece, piece, "up", go, z >= step + 1)
            got = z < depth - step
            falling[q].arrived()
            piece = whole.at[:, (z + step) * 2 + x]
            copy(piece, piece, "x", got, got)
            if step + 1 < depth:
                go = (z < depth - step) & (z > 0)
                falling[q] = copy(piece, piece, "down", go, z < depth - step - 1)
    copy.finish()
    for entry in local:
        entry.wait()


def gather(fsdp, weights, up_part, params, acts, spatial, cot):
    qkv_w, out_w, down_w, spatial_w = weights
    rows, width = acts.shape[2:]
    half, unit = width // 2, down_w.shape[2] // 2
    hbm = pl.BlockSpec(memory_space=pl.ANY)
    depth = fsdp // 2
    shapes = [
        (3, qkv_w.shape[3], half),
        (2, qkv_w.shape[3], half),
        (1, qkv_w.shape[3], half),
        params.shape,
        up_part.shape,
        (1, unit, width),
    ]
    copies = 7 + (3 + 4 * (depth - 1) - 2) * len(shapes)
    shapes = [jax.ShapeDtypeStruct((s[0], fsdp) + s[1:], BF16) for s in shapes]
    shapes += [jax.ShapeDtypeStruct((n, rows, width), BF16) for n in (4, 4, 2)]
    return pl.pallas_call(
        partial(gather_kernel, fsdp, (half, unit)),
        out_shape=shapes,
        in_specs=[hbm] * 9,
        out_specs=[hbm] * len(shapes),
        scratch_shapes=[
            pltpu.SemaphoreType.DMA((copies,)),
            pltpu.SemaphoreType.DMA((copies,)),
            pltpu.SemaphoreType.DMA((len(shapes),)),
        ],
        compiler_params=pltpu.CompilerParams(collective_id=0, has_side_effects=True),
        name="gather",
    )(qkv_w, out_w, down_w, spatial_w, up_part, params, acts, spatial, cot)


def gather_plain(weights, up_part, params, acts, spatial, cot, y, c):
    qkv_w, out_w, down_w, spatial_w = weights
    half, unit = acts.shape[3] // 2, down_w.shape[2] // 2

    def columns(array):
        return lax.dynamic_slice_in_dim(array, c * half, half, array.ndim - 1)

    shards = (
        columns(pick(qkv_w[0], y)),
        columns(spatial_w),
        columns(pick(out_w[0], y))[None],
        params,
        up_part,
        lax.dynamic_slice_in_dim(pick(down_w[0], y), c * unit, unit, 0)[None],
    )
    full = [lax.all_gather(s, "fsdp", axis=1) for s in shards]

    def own_blocks(value):
        return jnp.stack([pick(value, y)[0], y_swap(pick(value, 1 - y)[0])])

    x_own, s_own, c_own = own_blocks(acts), own_blocks(spatial), own_blocks(cot)
    x_all = jnp.concatenate([x_own, core_swap(x_own)])
    s_all = jnp.concatenate([s_own, core_swap(s_own)])
    return full + [x_all, s_all, c_own]


def add_rows(out, terms):
    size = out.shape[0]
    step = 16 if size % 16 == 0 else size

    def body(i, carry):
        at = pl.ds(pl.multiple_of(i * step, step), step)
        total = None
        for ref in terms:
            part = wide(ref[at, :])
            total = part if total is None else total + part
        out[at, :] = total.astype(out.dtype)
        return carry

    lax.fori_loop(0, size // step, body, 0)


def reduce_kernel(fsdp, count, *refs):
    grads, table = refs[:count], refs[count]
    results, table_out = refs[count + 1 : 2 * count + 1], refs[2 * count + 1]
    refs = refs[2 * count + 2 :]
    buffers = [refs[6 * q : 6 * q + 6] for q in range(count)]
    table_in, table_sum, send, recv, own = refs[6 * count :]
    at = places(fsdp)
    f, z, x, depth = at["f"], at["z"], at["x"], at["depth"]
    last = depth - 1
    copy = Sender(at, send, recv)
    peers = [((f + k) % fsdp, at["r"]) for k in range(1, fsdp)]
    greet(peers + [copy.devices["y"], copy.devices["c"]])
    state = [dict() for _ in range(count)]
    local = []

    def begin(q):
        g, x_in = grads[q], buffers[q][0]
        cross = state[q]["x"] = {}
        for d in range(last, 0, -1):
            for sign in (1, -1):
                target = z + sign * d
                ok = target <= last if sign > 0 else target >= 0
                cross[sign * d] = copy(g.at[target * 2 + 1 - x], x_in.at[target], "x", ok, ok)
        cross[0] = copy(g.at[at["other"]], x_in.at[z], "x")
        state[q]["up"], state[q]["down"] = {}, {}

    def outward(q, d):
        g, (x_in, from_low, from_high, to_high, to_low, _) = grads[q], buffers[q]
        s = state[q]
        for sign, arrive, leave, name in (
            (1, from_low, to_high, "up"),
            (-1, from_high, to_low, "down"),
        ):
            target = z + sign * d
            ok = target <= last if sign > 0 else target >= 0
            behind = z >= 1 if sign > 0 else z <= last - 1
            s["x"][sign * d].arrived()
            if d in s[name]:
                s[name][d].arrived()
                terms = (g.at[target * 2 + x], x_in.at[target])
                out = leave.at[d - 1]
                when(ok & behind, partial(add_rows, out, terms + (arrive.at[d],)))
                when(ok & jnp.logical_not(behind), partial(add_rows, out, terms))
            else:
                terms = (g.at[target * 2 + x], x_in.at[target])
                when(ok, partial(add_rows, leave.at[d - 1], terms))
            here = z + sign * (d - 1)
            got = behind & (here <= last if sign > 0 else here >= 0)
            s[name][d - 1] = copy(leave.at[d - 1], arrive.at[d - 1], name, ok, got)

    def own_sum(q):
        g, (x_in, from_low, from_high, _, _, total) = grads[q], buffers[q]
        res = results[q]
        s = state[q]
        s["x"][0].arrived()
        s["up"][0].arrived()
        s["down"][0].arrived()
        terms = (g.at[f], x_in.at[z])
        below, above = from_low.at[0], from_high.at[0]
        when(z == 0, partial(add_rows, total, terms + (above,)))
        when(z == last, partial(add_rows, total, terms + (below,)))
        when((z > 0) & (z < last), partial(add_rows, total, terms + (above, below)))
        s["y"] = copy(total, res.at[2], "y")
        copy(total, res.at[1], "c")
        local.append(pltpu.make_async_copy(total, res.at[0], own.at[q]))
        local[-1].start()

    def hand_on(q):
        state[q]["y"].arrived()
        copy(results[q].at[2], results[q].at[3], "c")

    tables = [copy(table, table_in.at[k], peers[k]) for k in range(fsdp - 1)]
    begin(0)
    for step in range(count + depth):
        if step + 1 < count:
            begin(step + 1)
        for stage in range(depth + 1):
            q = step - stage
            if not 0 <= q < count:
                continue
            if stage < last:
                outward(q, last - stage)
            elif stage == last:
                own_sum(q)
            else:
                hand_on(q)
        if step == 1:
            for entry in tables:
                entry.arrived()
            total = table[...]
            for k in range(fsdp - 1):
                total = total + table_in[k]
            table_sum[...] = total
            table_y = copy(table_sum, table_out.at[2], "y")
            copy(table_sum, table_out.at[1], "c")
            local.append(pltpu.make_async_copy(table_sum, table_out.at[0], own.at[count]))
            local[-1].start()
        if step == 2:
            table_y.arrived()
            copy(table_out.at[2], table_out.at[3], "c")
    copy.finish()
    for entry in local:
        entry.wait()


def reduce(fsdp, grads, table):
    count, depth = len(grads), fsdp // 2
    vmem, hbm = pl.BlockSpec(memory_space=pltpu.VMEM), pl.BlockSpec(memory_space=pl.ANY)
    scratch = []
    for g in grads:
        _, rows, cols = g.shape
        scratch += [pltpu.VMEM((n, rows, cols), BF16) for n in (depth,) + (depth - 1,) * 4]
        scratch.append(pltpu.VMEM((rows, cols), BF16))
    scratch += [pltpu.VMEM((fsdp - 1,) + table.shape, F32), pltpu.VMEM(table.shape, F32)]
    copies = (2 * (depth - 1) + 1 + 2 * (depth - 1) + 3) * count + fsdp - 1 + 3
    shapes = [jax.ShapeDtypeStruct((4,) + g.shape[1:], BF16) for g in grads]
    shapes.append(jax.ShapeDtypeStruct((4,) + table.shape, F32))
    return pl.pallas_call(
        partial(reduce_kernel, fsdp, count),
        out_shape=shapes,
        in_specs=[vmem] * (count + 1),
        out_specs=[hbm] * (count + 1),
        scratch_shapes=scratch
        + [
            pltpu.SemaphoreType.DMA((copies,)),
            pltpu.SemaphoreType.DMA((copies,)),
            pltpu.SemaphoreType.DMA((count + 1,)),
        ],
        compiler_params=pltpu.CompilerParams(
            collective_id=1, has_side_effects=True, vmem_limit_bytes=52 << 20
        ),
        name="reduce",
    )(*grads, table)


def reduce_plain(grads, table):
    results = []

    def spread(total):
        far = y_swap(total)
        return jnp.stack([total, core_swap(total), far, core_swap(far)])

    for g in grads:
        results.append(spread(lax.psum_scatter(g, "fsdp", scatter_dimension=0, tiled=True)[0]))
    results.append(spread(lax.psum(table, "fsdp")))
    return results


def finish_kernel(half, unit, down_r, up_r, qkv_r, sp_r, out_r, down, up, qkv, sp, out):
    r = lax.axis_index("rep")
    y, c = r // 2, r % 2
    for t in range(2):
        s = y if t == 0 else 1 - y
        for h in range(2):
            k = c if h == 0 else 1 - c
            place = pl.ds(pl.multiple_of(k * half, 128), half)
            part = 2 * t + h
            down[0, s, pl.ds(pl.multiple_of(k * unit, 16), unit), :] = wide(down_r[part])
            for j in range(3):
                qkv[0, s, j, :, place] = wide(qkv_r[part, :, j * half : (j + 1) * half])
            out[0, s, :, place] = wide(out_r[part, :, :half])
            if t == 0:
                total = wide(sp_r[h]) + wide(sp_r[2 + h])
                for j in range(2):
                    sp[j, :, place] = total[:, j * half : (j + 1) * half]
        mine, theirs = wide(up_r[2 * t]), wide(up_r[2 * t + 1])
        first = jnp.where(c == 0, mine, theirs)
        second = jnp.where(c == 0, theirs, mine)
        pieces = []
        for i in range(up_r.shape[2] // unit):
            pieces += [first[:, i * unit : (i + 1) * unit], second[:, i * unit : (i + 1) * unit]]
        up[0, s] = jnp.concatenate(pieces, axis=1)


def finish_plain(y, c, fsdp, reduced, shapes):
    down_r, up_r, qkv_r, sp_r, out_r = [wide(r) for r in reduced]
    rows, width = shapes[3][1:]
    half = width // 2

    def whole(parts, axis):
        streams = [ordered(c, parts[2 * s], parts[2 * s + 1], axis) for s in range(2)]
        return ordered(y, streams[0], streams[1], 0)

    down = whole(down_r, 0).reshape(shapes[0])
    up = whole(up_r.reshape(4, rows, fsdp, -1), 2).reshape(shapes[1])
    qkv = whole(qkv_r.reshape(4, rows, 3, half), 2)
    qkv = jnp.transpose(qkv.reshape(2, rows, 3, width), (0, 2, 1, 3))[None]
    out = whole(out_r[:, :, :half], 1).reshape(shapes[4])
    sp = (sp_r[:2] + sp_r[2:]).reshape(2, rows, 2, half)
    sp = ordered(c, sp[0], sp[1], 2).reshape(rows, 2, width)
    return down, up, qkv, jnp.transpose(sp, (1, 0, 2)), out


def finish(half, unit, reduced, shapes):
    vmem = pl.BlockSpec(memory_space=pltpu.VMEM)
    return pl.pallas_call(
        partial(finish_kernel, half, unit),
        out_shape=[jax.ShapeDtypeStruct(s, F32) for s in shapes],
        in_specs=[vmem] * 5,
        out_specs=[vmem] * 5,
        compiler_params=pltpu.CompilerParams(vmem_limit_bytes=32 << 20),
        name="finish",
    )(*reduced)


def pair_mask(lanes, head_width, t):
    lane = lax.broadcasted_iota(jnp.int32, (1, lanes), 1)
    return ((lane % 128) // head_width == t).astype(BF16)


def attention_kernel(head_width, scale, q, k, v, sq, sk, hot_ref, bias, mixed, probs):
    keys = jnp.concatenate([k[...], sk[...]], axis=1)
    queries = jnp.concatenate([q[...], sq[...]], axis=1) * scale
    hot = hot_ref[...]
    value = v[...]
    parts = []
    for t in range(128 // head_width):
        masked = queries * pair_mask(256, head_width, t)
        feature = low(dot(hot, bias[t]))
        scores = dot(keys, masked, 1, 1) + dot(hot, feature, 1, 1)
        top = jnp.max(scores, axis=0, keepdims=True)
        raised = jnp.exp(scores - top)
        prob = low(raised * (1.0 / jnp.sum(raised, axis=0, keepdims=True)))
        probs[t] = prob
        both = dot(value, prob, 0, 0)
        parts.append(both[t * head_width : (t + 1) * head_width])
    mixed[...] = low(jnp.transpose(jnp.concatenate(parts, axis=0)))


def attention(qkv, hot, bias, head_width):
    tokens = qkv[0].shape[0]
    heads = bias.shape[0]
    per = 128 // head_width
    groups = heads // per
    full = lambda g: (0, 0)
    pair = pl.BlockSpec((tokens, 128), lambda g: (0, g))
    return pl.pallas_call(
        partial(attention_kernel, head_width, head_width**-0.5),
        grid=(groups,),
        out_shape=(
            jax.ShapeDtypeStruct((tokens, heads * head_width), BF16),
            jax.ShapeDtypeStruct((heads, tokens, tokens), BF16),
        ),
        in_specs=[pair] * 5
        + [
            pl.BlockSpec(hot.shape, full),
            pl.BlockSpec((per,) + bias.shape[1:], lambda g: (g, 0, 0)),
        ],
        out_specs=[
            pair,
            pl.BlockSpec((per, tokens, tokens), lambda g: (g, 0, 0)),
        ],
        compiler_params=pltpu.CompilerParams(vmem_limit_bytes=48 << 20),
        name="attention",
    )(*qkv, hot, bias)


def attention_back_kernel(
    head_width, scale, groups, q, k, v, sq, sk, hot_ref, probs, mixed_grad, grad, sgrad, corner
):
    g = pl.program_id(0)
    keys = jnp.concatenate([k[...], sk[...]], axis=1)
    queries = jnp.concatenate([q[...], sq[...]], axis=1) * scale
    hot = hot_ref[...]
    value = v[...]
    outer = mixed_grad[...]
    key_total = value_total = None
    query_rows = [[], []]
    for t in range(128 // head_width):
        outer_t = outer * pair_mask(128, head_width, t)
        prob = probs[t]
        prob_wide = wide(prob)
        prob_grad = dot(value, outer_t, 1, 1)
        delta = jnp.sum(prob_wide * prob_grad, axis=0, keepdims=True)
        score_grad = low(prob_wide * (prob_grad - delta))
        value_part = dot(prob, outer_t)
        key_part = dot(score_grad, queries * pair_mask(256, head_width, t))
        key_total = key_part if t == 0 else key_total + key_part
        value_total = value_part if t == 0 else value_total + value_part
        query_t = dot(keys, score_grad, 0, 0)
        for half in range(2):
            start = half * 128 + t * head_width
            query_rows[half].append(query_t[start : start + head_width])
        feature_grad = dot(hot, score_grad, 0, 0)
        high = low(feature_grad)
        rest = low(feature_grad - wide(high))
        corner[t] = dot(high, hot) + dot(rest, hot)
    query_total = jnp.transpose(jnp.concatenate(query_rows[0] + query_rows[1], axis=0)) * scale

    def place(j):
        return pl.ds(pl.multiple_of(j * groups * 128 + g * 128, 128), 128)

    grad[:, place(0)] = low(query_total[:, :128])
    grad[:, place(1)] = low(key_total[:, :128])
    grad[:, place(2)] = low(value_total)
    sgrad[:, place(0)] = low(query_total[:, 128:])
    sgrad[:, place(1)] = low(key_total[:, 128:])


def attention_back(qkv, hot, probs, mixed_grad, head_width):
    tokens, own_width = qkv[0].shape
    heads = probs.shape[0]
    per = 128 // head_width
    groups = heads // per
    wide_hot = hot.shape[1]
    full = lambda g: (0, 0)
    pair = pl.BlockSpec((tokens, 128), lambda g: (0, g))
    return pl.pallas_call(
        partial(attention_back_kernel, head_width, head_width**-0.5, groups),
        grid=(groups,),
        out_shape=(
            jax.ShapeDtypeStruct((tokens, 3 * own_width), BF16),
            jax.ShapeDtypeStruct((tokens, 2 * own_width), BF16),
            jax.ShapeDtypeStruct((heads, wide_hot, wide_hot), F32),
        ),
        in_specs=[pair] * 5
        + [
            pl.BlockSpec(hot.shape, full),
            pl.BlockSpec((per, tokens, tokens), lambda g: (g, 0, 0)),
            pair,
        ],
        out_specs=[
            pl.BlockSpec((tokens, 3 * own_width), full),
            pl.BlockSpec((tokens, 2 * own_width), full),
            pl.BlockSpec((per, wide_hot, wide_hot), lambda g: (g, 0, 0)),
        ],
        compiler_params=pltpu.CompilerParams(vmem_limit_bytes=48 << 20),
        name="attention_back",
    )(*qkv, hot, probs, mixed_grad)


def norm_forward(residual, gain_row, bias_row):
    centre = residual - jnp.mean(residual, axis=-1, keepdims=True)
    inv_std = lax.rsqrt(jnp.mean(centre * centre, axis=-1, keepdims=True) + EPSILON)
    normed = centre * inv_std
    return normed * gain_row + bias_row, normed, inv_std


def norm_backward(grad_out, normed, inv_std, gain_row):
    scaled = grad_out * gain_row
    mean_one = jnp.mean(scaled, axis=-1, keepdims=True)
    mean_two = jnp.mean(scaled * normed, axis=-1, keepdims=True)
    grad_in = inv_std * (scaled - mean_one - normed * mean_two)
    return grad_in, jnp.sum(grad_out * normed, axis=0), jnp.sum(grad_out, axis=0)


def per_device(
    fsdp,
    activations,
    spatial,
    buckets,
    page_valid,
    qkv_w,
    out_w,
    up_w,
    down_w,
    spatial_w,
    tables,
    norm_gains,
    biases,
    cotangent,
):
    rows, width = activations.shape[2:]
    tokens = buckets.shape[3]
    heads = tables.shape[3]
    head_width = width // heads
    bins = (tables.shape[4] + 1) // 2
    own_heads = heads // 2
    own_width = width // 2
    shard_rows = qkv_w.shape[3]
    ff = up_w.shape[3]
    unit = ff // fsdp // 2
    own_ff = ff // 2
    rep = lax.axis_index("rep")
    y, c = rep // 2, rep % 2

    def columns(array, axis):
        return lax.dynamic_slice_in_dim(array, c * own_width, own_width, axis)

    params = jnp.concatenate([pick(norm_gains[0], y), pick(biases[0], y)])
    params = jnp.pad(params, ((0, 12), (0, -shard_rows % 128)))[None]
    up_part = pick(pick(up_w[0], y).reshape(shard_rows, fsdp, 2, unit), c, 2)
    up_part = up_part.reshape(1, shard_rows, own_ff)
    weights = (qkv_w, out_w, down_w, spatial_w)
    if fsdp == 8:
        gathered = gather(fsdp, weights, up_part, params, activations, spatial, cotangent)
    else:
        gathered = gather_plain(weights, up_part, params, activations, spatial, cotangent, y, c)
    norms = gathered[3][0]
    gathered = [g.reshape(g.shape[0], -1, g.shape[3]) for g in gathered[:3] + gathered[4:6]] + [
        g.reshape(-1, width) for g in gathered[6:]
    ]
    w_qkv, w_spatial, (w_out,), (w_up,), (w_down,), x_all, s_all, cot = gathered
    own = tokens // 2
    block = rows

    norms = wide(jnp.transpose(norms[:, :4, :shard_rows], (1, 0, 2)).reshape(4, 1, width))
    gain_one, gain_two, bias_one, bias_two = [norms[i] for i in range(4)]
    mine = lax.dynamic_slice(w_out, (c * own_width, 0), (own_width, own_width))
    give = lax.dynamic_slice(w_out, ((1 - c) * own_width, 0), (own_width, own_width))
    w_own = ordered(c, mine, core_swap(give), 1).reshape(own_width, width)

    page_buckets = pick(buckets, y)[:, 0].reshape(3, 4, block)
    order = [rep, y_of(rep), c_of(rep), y_of(c_of(rep))]
    page_buckets = jnp.concatenate([pick(page_buckets, i, 1) for i in order], axis=1)
    hot = (page_buckets[..., None] == jnp.arange(bins, dtype=jnp.int32)).astype(BF16)
    hot = jnp.transpose(hot, (1, 0, 2)).reshape(tokens, 3 * bins)
    left = lax.broadcasted_iota(jnp.int32, (bins, bins, 2 * bins - 1), 0)
    right = lax.broadcasted_iota(jnp.int32, (bins, bins, 2 * bins - 1), 1)
    slot = lax.broadcasted_iota(jnp.int32, (bins, bins, 2 * bins - 1), 2)
    offsets = (left - right + bins - 1 == slot).astype(F32)
    own_tables = lax.dynamic_slice_in_dim(pick(tables[0], y), c * own_heads, own_heads, 1)
    matrices = jnp.einsum("khr,uvr->hkuv", wide(own_tables), offsets, precision=HIGHEST)
    bias = jnp.einsum("hkuv,kq->hkuqv", matrices, jnp.eye(3, dtype=F32), precision=HIGHEST)
    bias = low(bias.reshape(own_heads, 3 * bins, 3 * bins))

    valid = page_valid[0] > 0
    x_own = wide(x_all[:own])
    qkv = [low(dot(x_all, w_qkv[j])) for j in range(3)] + [
        low(dot(s_all, w_spatial[j])) for j in range(2)
    ]
    mixed, probs = attention(qkv, hot, bias, head_width)

    def core_sum(partial_sum):
        return partial_sum[:own] + wide(core_swap(low(partial_sum[own:])))

    def both_cores(value):
        return jnp.concatenate([value, core_swap(value)])

    def other_stream(value):
        sent = low(value)
        return wide(y_swap(jnp.concatenate([sent[block:], sent[:block]])))

    branch = core_sum(dot(mixed, w_own))
    residual = x_own + (branch + other_stream(branch))
    hidden, normed_one, inv_one = norm_forward(residual, gain_one, bias_one)
    hidden_all = both_cores(low(hidden))
    gate = dot(hidden_all, w_up)
    active = low(jax.nn.gelu(gate, approximate=True))
    ffn = core_sum(dot(active, w_down))
    result, normed_two, inv_two = norm_forward(hidden + ffn, gain_two, bias_two)
    layer_out = low(jnp.where(valid, result, x_own))
    layer_out = ordered(y, layer_out[:block], y_swap(layer_out[block:]), 0)[:, None]

    upstream = jnp.where(valid, wide(cot), 0.0)
    back_two, gain_two_grad, bias_two_grad = norm_backward(upstream, normed_two, inv_two, gain_two)
    ffn_grad = both_cores(low(back_two))
    down_grad = low(dot(active, ffn_grad, 0, 0))
    active_grad = dot(ffn_grad, w_down, 1, 1)
    pull = jax.vjp(partial(jax.nn.gelu, approximate=True), gate)[1]
    gate_grad = low(pull(active_grad)[0])
    up_grad = low(dot(hidden_all, gate_grad, 0, 0))
    hidden_grad = back_two + core_sum(dot(gate_grad, w_up, 1, 1))
    back_one, gain_one_grad, bias_one_grad = norm_backward(
        hidden_grad, normed_one, inv_one, gain_one
    )
    branch_grad = both_cores(low(back_one + other_stream(back_one)))
    mixed_grad = low(dot(branch_grad, w_own, 1, 1))
    out_own = low(dot(mixed, branch_grad, 0, 0))
    out_kept = columns(out_own, 1)
    out_given = lax.dynamic_slice_in_dim(out_own, (1 - c) * own_width, own_width, 1)
    out_grad = ordered(c, out_kept, core_swap(out_given), 0).reshape(width, own_width)
    norm_grads = jnp.stack([gain_one_grad, gain_two_grad, bias_one_grad, bias_two_grad], 1)
    out_grad = jnp.concatenate([out_grad, jnp.pad(low(norm_grads), ((0, 0), (0, 124)))], axis=1)
    grad, sgrad, corner = attention_back(qkv, hot, probs, mixed_grad, head_width)
    qkv_grad = low(dot(x_all, grad, 0, 0))
    spatial_grad = low(dot(s_all, sgrad, 0, 0))
    back = sum(
        dot(grad[:, j * own_width : (j + 1) * own_width], w_qkv[j], 1, 1) for j in range(3)
    )
    in_own = back_one + core_sum(back)
    in_own = jnp.where(valid, in_own, wide(cot))
    in_far = wide(y_swap(low(in_own[block:])))
    in_grad = ordered(y, in_own[:block], in_far, 0)[:, None]

    corner = corner.reshape(own_heads, 3, bins, 3, bins)
    corner = jnp.stack([corner[:, k, :, k, :] for k in range(3)])
    table = jnp.einsum("khvu,uvr->khr", corner, offsets, precision=HIGHEST)
    flat = own_heads * (2 * bins - 1)
    table = jnp.pad(table.reshape(3, flat), ((0, 5), (0, -flat % 128)))

    grads = [
        g.reshape(fsdp, -1, g.shape[1])
        for g in (down_grad, up_grad, qkv_grad, spatial_grad, out_grad)
    ]
    shapes = (down_w.shape, up_w.shape, qkv_w.shape, spatial_w.shape, out_w.shape)
    if fsdp == 8:
        reduced = reduce(fsdp, grads, table)
        finished = finish(own_width, unit, reduced[:5], shapes)
    else:
        reduced = reduce_plain(grads, table)
        finished = finish_plain(y, c, fsdp, reduced[:5], shapes)
    down_grad, up_grad, qkv_grad, spatial_grad, out_grad = finished
    table = reduced[5][:, :3, :flat].reshape(4, 3, own_heads, -1)
    table = [ordered(c, table[2 * s], table[2 * s + 1], 1) for s in range(2)]
    table_grad = ordered(y, table[0], table[1], 0).reshape(tables.shape)
    norm_sum = wide(reduced[4][:, :, own_width : own_width + 4])
    norm_sum = jnp.transpose(norm_sum[0::2] + norm_sum[1::2], (0, 2, 1))
    norm_sum = ordered(y, norm_sum[0], norm_sum[1], 0)
    gain_grad, bias_grad = norm_sum[None, :, :2], norm_sum[None, :, 2:]
    return (
        layer_out,
        in_grad,
        qkv_grad,
        out_grad,
        up_grad,
        down_grad,
        spatial_grad,
        table_grad,
        gain_grad,
        bias_grad,
    )


def y_of(rep):
    return (rep + 2) % 4


def c_of(rep):
    return rep + 1 - 2 * (rep % 2)


def solution(mesh):
    weight = P(None, None, "fsdp", None)
    tokens = P(None, "fsdp", "rep", None)
    qkv = P(None, None, None, "fsdp", None)
    norm = P(None, None, None, "fsdp")
    return jax.shard_map(
        partial(per_device, mesh.shape["fsdp"]),
        mesh=mesh,
        in_specs=(
            tokens,
            tokens,
            weight,
            P("fsdp"),
            qkv,
            weight,
            weight,
            weight,
            P(None, "fsdp", None),
            P(),
            norm,
            norm,
            tokens,
        ),
        out_specs=(
            tokens,
            tokens,
            qkv,
            weight,
            weight,
            weight,
            P(None, "fsdp", None),
            P(),
            norm,
            norm,
        ),
        check_vma=False,
    )
```

```python
from functools import partial

import jax
import jax.numpy as jnp
from jax import lax
from jax.experimental import pallas as pl
from jax.experimental.pallas import tpu as pltpu
from jax.sharding import PartitionSpec as P

EPSILON = 1e-05
HIGHEST = lax.Precision.HIGHEST
F32 = jnp.float32
BF16 = jnp.bfloat16
MESH = pl.DeviceIdType.MESH


def low(value):
    return value.astype(BF16)


def wide(value):
    return value.astype(F32)


def dot(left, right, left_axis=1, right_axis=0, precision=None):
    dims = (((left_axis,), (right_axis,)), ((), ()))
    return lax.dot_general(left, right, dims, precision=precision, preferred_element_type=F32)


def pick(array, index, axis=0):
    return lax.dynamic_index_in_dim(array, index, axis, keepdims=False)


def core_swap(value):
    return lax.ppermute(value, "rep", [(0, 1), (1, 0), (2, 3), (3, 2)])


def y_swap(value):
    return lax.ppermute(value, "rep", [(0, 2), (2, 0), (1, 3), (3, 1)])


def ordered(flag, first, second, axis):
    return jnp.where(
        flag == 0,
        jnp.stack([first, second], axis),
        jnp.stack([second, first], axis),
    )


def places(fsdp):
    f = lax.axis_index("fsdp")
    r = lax.axis_index("rep")
    y, c = r // 2, r % 2
    return dict(
        f=f,
        r=r,
        y=y,
        c=c,
        z=f // 2,
        x=f % 2,
        depth=fsdp // 2,
        other=f + 1 - 2 * (f % 2),
        up=(f + 2) % fsdp,
        down=(f + fsdp - 2) % fsdp,
        r_y=(1 - y) * 2 + c,
        r_c=y * 2 + 1 - c,
    )


def greet(partners):
    barrier = pltpu.get_barrier_semaphore()
    for partner in partners:
        pl.semaphore_signal(barrier, inc=1, device_id=partner, device_id_type=MESH)
    pl.semaphore_wait(barrier, len(partners))


def when(condition, action):
    if condition is None:
        action()
    else:
        pl.when(condition)(action)


class Entry:
    def __init__(self, copy, sent, got):
        self.copy, self.sent, self.got = copy, sent, got
        self.seen = False

    def start(self):
        when(self.sent, self.copy.start)

    def arrived(self):
        if not self.seen:
            self.seen = True
            when(self.got, self.copy.wait_recv)


class Sender:
    def __init__(self, at, send, recv):
        self.send, self.recv = send, recv
        self.entries = []
        self.devices = {
            "x": (at["other"], at["r"]),
            "up": (at["up"], at["r"]),
            "down": (at["down"], at["r"]),
            "y": (at["f"], at["r_y"]),
            "c": (at["f"], at["r_c"]),
        }

    def make(self, source, target, where, sent=None, got=None):
        k = len(self.entries)
        copy = pltpu.make_async_remote_copy(
            src_ref=source,
            dst_ref=target,
            send_sem=self.send.at[k],
            recv_sem=self.recv.at[k],
            device_id=self.devices[where] if isinstance(where, str) else where,
            device_id_type=MESH,
        )
        self.entries.append(Entry(copy, sent, got))
        return self.entries[-1]

    def __call__(self, *given, **named):
        entry = self.make(*given, **named)
        entry.start()
        return entry

    def finish(self):
        for entry in self.entries:
            entry.arrived()
        for entry in self.entries:
            when(entry.sent, entry.copy.wait_send)


def copy_rows(refs, target, step, action):
    def body(i, carry):
        at = pl.ds(pl.multiple_of(i * step, step), step)
        target[at, :] = action(*[ref[at, :] for ref in refs]).astype(target.dtype)
        return carry

    lax.fori_loop(0, target.shape[0] // step, body, 0)


def flat(value):
    return value.reshape(-1, value.shape[-1])


def forward_kernel(fsdp, sizes, *refs):
    qkv_w, out_w, down_w, spatial_w, up_part, params, acts, spatial, cot = refs[:9]
    hot_ref, bias_ref, valid = refs[9:12]
    full, (x_all, s_all, c_own) = refs[12:18], refs[18:21]
    proj, probs, mixed, w_own, hidden_all, gate, active = refs[21:28]
    normed_one, inv_one, normed_two, inv_two, layer_out = refs[28:33]
    w_given, rows_out, rows_in, branch, y_out, y_in, hidden, rows_out2, rows_in2, result = refs[
        33:43
    ]
    send, recv, own = refs[43:]
    w_qkv, w_spatial, w_out, norms, w_up, w_down = full
    at = places(fsdp)
    y, c, f, z, x, depth = [at[k] for k in ("y", "c", "f", "z", "x", "depth")]
    copy = Sender(at, send, recv)
    greet(list(copy.devices.values()))
    half, unit, head_width = sizes
    quarter = fsdp // 2
    columns = pl.ds(pl.multiple_of(c * half, 128), half)
    others = pl.ds(pl.multiple_of((1 - c) * half, 128), half)
    shards = (
        qkv_w.at[0, y, :, :, columns],
        spatial_w.at[:, :, columns],
        out_w.at[0, pl.ds(y, 1), :, columns],
        params,
        up_part,
        down_w.at[0, pl.ds(y, 1), pl.ds(pl.multiple_of(c * unit, 16), unit), :],
    )
    local = []
    across = {}

    def keep(source, target):
        local.append(pltpu.make_async_copy(source, target, own.at[len(local)]))
        local[-1].start()
        return local[-1]

    rising, falling = [None] * len(full), [None] * len(full)

    def begin(q):
        shard, whole = shards[q], full[q]
        across[q] = [copy(shard, whole.at[:, f], "x")]
        rising[q] = copy(shard, whole.at[:, f], "up", z < depth - 1, z > 0)
        falling[q] = copy(shard, whole.at[:, f], "down", z > 0, z < depth - 1)
        keep(shard, whole.at[:, f])

    def advance(q, step):
        whole = full[q]
        got = z >= step
        rising[q].arrived()
        piece = whole.at[:, (z - step) * 2 + x]
        across[q].append(copy(piece, piece, "x", got, got))
        if step + 1 < depth:
            go = (z >= step) & (z < depth - 1)
            rising[q] = copy(piece, piece, "up", go, z >= step + 1)
        got = z < depth - step
        falling[q].arrived()
        piece = whole.at[:, (z + step) * 2 + x]
        across[q].append(copy(piece, piece, "x", got, got))
        if step + 1 < depth:
            go = (z < depth - step) & (z > 0)
            falling[q] = copy(piece, piece, "down", go, z < depth - step - 1)

    def complete(q):
        for entry in across[q]:
            entry.arrived()

    swaps = []
    for source, target in ((acts, x_all), (spatial, s_all)):
        swaps.append((copy(source.at[1 - y, 0], target.at[1], "y"), target))
        swaps[-1] += (copy(source.at[y, 0], target.at[2], "c"),)
        keep(source.at[y, 0], target.at[0])
    first, second = (0, 1, 2, 3), (4, 5)
    for q in first:
        begin(q)
    copy(cot.at[1 - y, 0], c_own.at[1], "y")
    keep(cot.at[y, 0], c_own.at[0])
    tokens_in = []
    for swap, target, near in swaps:
        swap.arrived()
        tokens_in += [near, copy(target.at[1], target.at[3], "c")]
    for step in range(1, depth):
        for q in first:
            advance(q, step)
    for q in second:
        begin(q)
    for entry in local:
        entry.wait()
    for entry in tokens_in:
        entry.arrived()

    complete(2)
    give = w_out.at[0, pl.ds((1 - c) * quarter, quarter)]
    given = copy(give, w_given, "c")
    complete(0)

    def project(source, weight, base):
        def body(j, carry):
            proj[base + j] = low(dot(flat(source[...]), flat(weight[j])))
            return carry

        return body

    lax.fori_loop(0, 3, project(x_all, w_qkv, 0), 0)
    complete(1)
    lax.fori_loop(0, 2, project(s_all, w_spatial, 3), 0)
    for q in second:
        advance(q, 1)

    per = 128 // head_width

    def heads(g, carry):
        lanes = pl.ds(pl.multiple_of(g * 128, 128), 128)
        group = pl.ds(g * per, per)
        attention_kernel(
            head_width,
            head_width**-0.5,
            *[proj.at[j, :, lanes] for j in range(5)],
            hot_ref,
            bias_ref.at[group],
            mixed.at[:, lanes],
            probs.at[group],
        )
        return carry

    lax.fori_loop(0, half // 128, heads, 0)

    w_own[:, columns] = flat(w_out[0, pl.ds(c * quarter, quarter)])
    given.arrived()
    w_own[:, others] = flat(w_given[...])
    count = hidden.shape[0]
    block = count // 2
    mine, theirs = pl.ds(0, count), pl.ds(count, count)
    weight = w_own[...]
    rows_out[...] = low(dot(mixed[theirs, :], weight))
    swapped = copy(rows_out, rows_in, "c")
    branch[...] = dot(mixed[mine, :], weight)
    for q in second:
        advance(q, 2)
    swapped.arrived()
    crossed = []
    for i in range(2):
        part = pl.ds(i * block, block)
        branch_part = branch.at[part]

        def add(own_rows, other_rows):
            return own_rows + wide(other_rows)

        copy_rows((branch_part, rows_in.at[part]), branch_part, 32, add)
        copy_rows((branch_part,), y_out.at[i], 32, low)
        crossed.append(copy(y_out.at[i], y_in.at[1 - i], "y"))
    complete(3)
    table = jnp.concatenate([norms[0, i, :4, : half // quarter] for i in range(fsdp)], axis=1)
    table = wide(table)
    gain_one, gain_two, bias_one, bias_two = [table[i : i + 1] for i in range(4)]

    def norm_rows(source, gain_row, bias_row, normed, inv, target, size, start):
        step = 32

        def body(i, carry):
            rows = pl.ds(pl.multiple_of(i * step, step), step)
            out = pl.ds(pl.multiple_of(start + i * step, step), step)
            value, middle, scale = norm_forward(source(rows, out), gain_row, bias_row)
            normed[out, :] = middle
            inv[out, :] = jnp.broadcast_to(scale, (step, inv.shape[1]))
            target[out, :] = value
            return carry

        lax.fori_loop(0, size // step, body, 0)

    for i in (1, 0):
        crossed[1 - i].arrived()
        norm_rows(
            lambda rows, out, i=i: wide(x_all[i, rows, :]) + branch[out, :] + wide(y_in[i, rows, :]),
            gain_one,
            bias_one,
            normed_one,
            inv_one,
            hidden,
            block,
            i * block,
        )
    copy_rows((hidden,), hidden_all.at[mine], 32, low)
    swapped = copy(hidden_all.at[mine], hidden_all.at[theirs], "c")
    for q in second:
        advance(q, 3)

    swapped.arrived()
    complete(4)
    tile = half

    def rise(j, carry):
        lanes = pl.ds(pl.multiple_of(j * tile, 128), tile)
        value = dot(hidden_all[...], flat(w_up[0, :, :, lanes]))
        gate[:, lanes] = value
        active[:, lanes] = low(jax.nn.gelu(value, approximate=True))
        return carry

    lax.fori_loop(0, active.shape[1] // tile, rise, 0)
    complete(5)

    def fall(rows, target):
        def body(j, carry):
            lanes = pl.ds(pl.multiple_of(j * tile, 128), tile)
            weight = flat(w_down[0, :, :, lanes])
            target[:, lanes] = dot(active[rows, :], weight).astype(target.dtype)
            return carry

        lax.fori_loop(0, target.shape[1] // tile, body, 0)

    fall(theirs, rows_out2)
    swapped = copy(rows_out2, rows_in2, "c")
    fall(mine, branch)
    swapped.arrived()
    norm_rows(
        lambda rows, out: hidden[out, :] + branch[out, :] + wide(rows_in2[out, :]),
        gain_two,
        bias_two,
        normed_two,
        inv_two,
        branch,
        count,
        0,
    )
    keep_page = valid[0:1, 0:1] > 0
    for i in (1, 0):
        target = result if i == 1 else layer_out.at[y]
        copy_rows(
            (branch.at[pl.ds(i * block, block)], x_all.at[i]),
            target,
            32,
            lambda value, before: jnp.where(keep_page, value, wide(before)),
        )
        if i == 1:
            copy(result, layer_out.at[y], "y")
    copy.finish()


def forward(fsdp, head_width, weights, up_part, params, acts, spatial, cot, hot, bias, valid):
    qkv_w, out_w, down_w, spatial_w = weights
    rows, width = acts.shape[2:]
    half, unit = width // 2, down_w.shape[2] // 2
    tokens, count = 4 * rows, 2 * rows
    own_ff = up_part.shape[2]
    shard = qkv_w.shape[3]
    heads = bias.shape[0]
    hbm, vmem = pl.BlockSpec(memory_space=pl.ANY), pl.BlockSpec(memory_space=pltpu.VMEM)
    shapes = [(3, shard, half), (2, shard, half), (1, shard, half), params.shape, up_part.shape]
    shapes.append((1, unit, width))
    shapes = [((s[0], fsdp) + s[1:], BF16) for s in shapes]
    shapes += [((n, rows, width), BF16) for n in (4, 4, 2)]
    shapes += [
        ((5, tokens, half), BF16),
        ((heads, tokens, tokens), BF16),
        ((tokens, half), BF16),
        ((half, width), BF16),
        ((tokens, width), BF16),
        ((tokens, own_ff), F32),
        ((tokens, own_ff), BF16),
        ((count, width), F32),
        ((count, 128), F32),
        ((count, width), F32),
        ((count, 128), F32),
        ((2, rows, width), BF16),
    ]
    return pl.pallas_call(
        partial(forward_kernel, fsdp, (half, unit, head_width)),
        out_shape=[jax.ShapeDtypeStruct(*s) for s in shapes],
        in_specs=[hbm] * 9 + [vmem] * 3,
        out_specs=[vmem] * len(shapes),
        scratch_shapes=[
            pltpu.VMEM((fsdp // 2, shard, half), BF16),
            pltpu.VMEM((count, width), BF16),
            pltpu.VMEM((count, width), BF16),
            pltpu.VMEM((count, width), F32),
            pltpu.VMEM((2, rows, width), BF16),
            pltpu.VMEM((2, rows, width), BF16),
            pltpu.VMEM((count, width), F32),
            pltpu.VMEM((count, width), BF16),
            pltpu.VMEM((count, width), BF16),
            pltpu.VMEM((rows, width), BF16),
            pltpu.SemaphoreType.DMA((100,)),
            pltpu.SemaphoreType.DMA((100,)),
            pltpu.SemaphoreType.DMA((9,)),
        ],
        compiler_params=pltpu.CompilerParams(
            collective_id=0, has_side_effects=True, vmem_limit_bytes=56 << 20
        ),
        name="forward",
    )(qkv_w, out_w, down_w, spatial_w, up_part, params, acts, spatial, cot, hot, bias, valid)


def gather_plain(weights, up_part, params, acts, spatial, cot, y, c):
    qkv_w, out_w, down_w, spatial_w = weights
    half, unit = acts.shape[3] // 2, down_w.shape[2] // 2

    def columns(array):
        return lax.dynamic_slice_in_dim(array, c * half, half, array.ndim - 1)

    shards = (
        columns(pick(qkv_w[0], y)),
        columns(spatial_w),
        columns(pick(out_w[0], y))[None],
        params,
        up_part,
        lax.dynamic_slice_in_dim(pick(down_w[0], y), c * unit, unit, 0)[None],
    )
    full = [lax.all_gather(s, "fsdp", axis=1) for s in shards]

    def own_blocks(value):
        return jnp.stack([pick(value, y)[0], y_swap(pick(value, 1 - y)[0])])

    x_own, s_own, c_own = own_blocks(acts), own_blocks(spatial), own_blocks(cot)
    x_all = jnp.concatenate([x_own, core_swap(x_own)])
    s_all = jnp.concatenate([s_own, core_swap(s_own)])
    return full + [x_all, s_all, c_own]


def add_rows(out, terms):
    size = out.shape[0]
    step = 16 if size % 16 == 0 else size

    def body(i, carry):
        at = pl.ds(pl.multiple_of(i * step, step), step)
        total = None
        for ref in terms:
            part = wide(ref[at, :])
            total = part if total is None else total + part
        out[at, :] = total.astype(out.dtype)
        return carry

    lax.fori_loop(0, size // step, body, 0)


def reduce_kernel(fsdp, count, *refs):
    grads, table = refs[:count], refs[count]
    results, table_out = refs[count + 1 : 2 * count + 1], refs[2 * count + 1]
    refs = refs[2 * count + 2 :]
    buffers = [refs[6 * q : 6 * q + 6] for q in range(count)]
    table_in, table_sum, send, recv, own = refs[6 * count :]
    at = places(fsdp)
    f, z, x, depth = at["f"], at["z"], at["x"], at["depth"]
    last = depth - 1
    copy = Sender(at, send, recv)
    peers = [((f + k) % fsdp, at["r"]) for k in range(1, fsdp)]
    greet(peers + [copy.devices["y"], copy.devices["c"]])
    state = [dict() for _ in range(count)]
    local = []

    def begin(q):
        g, x_in = grads[q], buffers[q][0]
        cross = state[q]["x"] = {}
        for d in range(last, 0, -1):
            for sign in (1, -1):
                target = z + sign * d
                ok = target <= last if sign > 0 else target >= 0
                cross[sign * d] = copy(g.at[target * 2 + 1 - x], x_in.at[target], "x", ok, ok)
        cross[0] = copy(g.at[at["other"]], x_in.at[z], "x")
        state[q]["up"], state[q]["down"] = {}, {}

    def outward(q, d):
        g, (x_in, from_low, from_high, to_high, to_low, _) = grads[q], buffers[q]
        s = state[q]
        for sign, arrive, leave, name in (
            (1, from_low, to_high, "up"),
            (-1, from_high, to_low, "down"),
        ):
            target = z + sign * d
            ok = target <= last if sign > 0 else target >= 0
            behind = z >= 1 if sign > 0 else z <= last - 1
            s["x"][sign * d].arrived()
            if d in s[name]:
                s[name][d].arrived()
                terms = (g.at[target * 2 + x], x_in.at[target])
                out = leave.at[d - 1]
                when(ok & behind, partial(add_rows, out, terms + (arrive.at[d],)))
                when(ok & jnp.logical_not(behind), partial(add_rows, out, terms))
            else:
                terms = (g.at[target * 2 + x], x_in.at[target])
                when(ok, partial(add_rows, leave.at[d - 1], terms))
            here = z + sign * (d - 1)
            got = behind & (here <= last if sign > 0 else here >= 0)
            s[name][d - 1] = copy(leave.at[d - 1], arrive.at[d - 1], name, ok, got)

    def own_sum(q):
        g, (x_in, from_low, from_high, _, _, total) = grads[q], buffers[q]
        res = results[q]
        s = state[q]
        s["x"][0].arrived()
        s["up"][0].arrived()
        s["down"][0].arrived()
        terms = (g.at[f], x_in.at[z])
        below, above = from_low.at[0], from_high.at[0]
        when(z == 0, partial(add_rows, total, terms + (above,)))
        when(z == last, partial(add_rows, total, terms + (below,)))
        when((z > 0) & (z < last), partial(add_rows, total, terms + (above, below)))
        s["y"] = copy(total, res.at[2], "y")
        copy(total, res.at[1], "c")
        local.append(pltpu.make_async_copy(total, res.at[0], own.at[q]))
        local[-1].start()

    def hand_on(q):
        state[q]["y"].arrived()
        copy(results[q].at[2], results[q].at[3], "c")

    tables = [copy(table, table_in.at[k], peers[k]) for k in range(fsdp - 1)]
    begin(0)
    for step in range(count + depth):
        if step + 1 < count:
            begin(step + 1)
        for stage in range(depth + 1):
            q = step - stage
            if not 0 <= q < count:
                continue
            if stage < last:
                outward(q, last - stage)
            elif stage == last:
                own_sum(q)
            else:
                hand_on(q)
        if step == 1:
            for entry in tables:
                entry.arrived()
            total = table[...]
            for k in range(fsdp - 1):
                total = total + table_in[k]
            table_sum[...] = total
            table_y = copy(table_sum, table_out.at[2], "y")
            copy(table_sum, table_out.at[1], "c")
            local.append(pltpu.make_async_copy(table_sum, table_out.at[0], own.at[count]))
            local[-1].start()
        if step == 2:
            table_y.arrived()
            copy(table_out.at[2], table_out.at[3], "c")
    copy.finish()
    for entry in local:
        entry.wait()


def reduce(fsdp, grads, table):
    count, depth = len(grads), fsdp // 2
    vmem, hbm = pl.BlockSpec(memory_space=pltpu.VMEM), pl.BlockSpec(memory_space=pl.ANY)
    scratch = []
    for g in grads:
        _, rows, cols = g.shape
        scratch += [pltpu.VMEM((n, rows, cols), BF16) for n in (depth,) + (depth - 1,) * 4]
        scratch.append(pltpu.VMEM((rows, cols), BF16))
    scratch += [pltpu.VMEM((fsdp - 1,) + table.shape, F32), pltpu.VMEM(table.shape, F32)]
    copies = (2 * (depth - 1) + 1 + 2 * (depth - 1) + 3) * count + fsdp - 1 + 3
    shapes = [jax.ShapeDtypeStruct((4,) + g.shape[1:], BF16) for g in grads]
    shapes.append(jax.ShapeDtypeStruct((4,) + table.shape, F32))
    return pl.pallas_call(
        partial(reduce_kernel, fsdp, count),
        out_shape=shapes,
        in_specs=[vmem] * (count + 1),
        out_specs=[hbm] * (count + 1),
        scratch_shapes=scratch
        + [
            pltpu.SemaphoreType.DMA((copies,)),
            pltpu.SemaphoreType.DMA((copies,)),
            pltpu.SemaphoreType.DMA((count + 1,)),
        ],
        compiler_params=pltpu.CompilerParams(
            collective_id=1, has_side_effects=True, vmem_limit_bytes=52 << 20
        ),
        name="reduce",
    )(*grads, table)


def reduce_plain(grads, table):
    results = []

    def spread(total):
        far = y_swap(total)
        return jnp.stack([total, core_swap(total), far, core_swap(far)])

    for g in grads:
        results.append(spread(lax.psum_scatter(g, "fsdp", scatter_dimension=0, tiled=True)[0]))
    results.append(spread(lax.psum(table, "fsdp")))
    return results


def finish_kernel(half, unit, down_r, up_r, qkv_r, sp_r, out_r, down, up, qkv, sp, out):
    r = lax.axis_index("rep")
    y, c = r // 2, r % 2
    for t in range(2):
        s = y if t == 0 else 1 - y
        for h in range(2):
            k = c if h == 0 else 1 - c
            place = pl.ds(pl.multiple_of(k * half, 128), half)
            part = 2 * t + h
            down[0, s, pl.ds(pl.multiple_of(k * unit, 16), unit), :] = wide(down_r[part])
            for j in range(3):
                qkv[0, s, j, :, place] = wide(qkv_r[part, :, j * half : (j + 1) * half])
            out[0, s, :, place] = wide(out_r[part, :, :half])
            if t == 0:
                total = wide(sp_r[h]) + wide(sp_r[2 + h])
                for j in range(2):
                    sp[j, :, place] = total[:, j * half : (j + 1) * half]
        mine, theirs = wide(up_r[2 * t]), wide(up_r[2 * t + 1])
        first = jnp.where(c == 0, mine, theirs)
        second = jnp.where(c == 0, theirs, mine)
        pieces = []
        for i in range(up_r.shape[2] // unit):
            pieces += [first[:, i * unit : (i + 1) * unit], second[:, i * unit : (i + 1) * unit]]
        up[0, s] = jnp.concatenate(pieces, axis=1)


def finish_plain(y, c, fsdp, reduced, shapes):
    down_r, up_r, qkv_r, sp_r, out_r = [wide(r) for r in reduced]
    rows, width = shapes[3][1:]
    half = width // 2

    def whole(parts, axis):
        streams = [ordered(c, parts[2 * s], parts[2 * s + 1], axis) for s in range(2)]
        return ordered(y, streams[0], streams[1], 0)

    down = whole(down_r, 0).reshape(shapes[0])
    up = whole(up_r.reshape(4, rows, fsdp, -1), 2).reshape(shapes[1])
    qkv = whole(qkv_r.reshape(4, rows, 3, half), 2)
    qkv = jnp.transpose(qkv.reshape(2, rows, 3, width), (0, 2, 1, 3))[None]
    out = whole(out_r[:, :, :half], 1).reshape(shapes[4])
    sp = (sp_r[:2] + sp_r[2:]).reshape(2, rows, 2, half)
    sp = ordered(c, sp[0], sp[1], 2).reshape(rows, 2, width)
    return down, up, qkv, jnp.transpose(sp, (1, 0, 2)), out


def finish(half, unit, reduced, shapes):
    vmem = pl.BlockSpec(memory_space=pltpu.VMEM)
    return pl.pallas_call(
        partial(finish_kernel, half, unit),
        out_shape=[jax.ShapeDtypeStruct(s, F32) for s in shapes],
        in_specs=[vmem] * 5,
        out_specs=[vmem] * 5,
        compiler_params=pltpu.CompilerParams(vmem_limit_bytes=32 << 20),
        name="finish",
    )(*reduced)


def pair_mask(lanes, head_width, t):
    lane = lax.broadcasted_iota(jnp.int32, (1, lanes), 1)
    return ((lane % 128) // head_width == t).astype(BF16)


def attention_kernel(head_width, scale, q, k, v, sq, sk, hot_ref, bias, mixed, probs):
    keys = jnp.concatenate([k[...], sk[...]], axis=1)
    queries = jnp.concatenate([q[...], sq[...]], axis=1) * scale
    hot = hot_ref[...]
    value = v[...]
    parts = []
    for t in range(128 // head_width):
        masked = queries * pair_mask(256, head_width, t)
        feature = low(dot(hot, bias[t]))
        scores = dot(keys, masked, 1, 1) + dot(hot, feature, 1, 1)
        top = jnp.max(scores, axis=0, keepdims=True)
        raised = jnp.exp(scores - top)
        prob = low(raised * (1.0 / jnp.sum(raised, axis=0, keepdims=True)))
        probs[t] = prob
        both = dot(value, prob, 0, 0)
        parts.append(both[t * head_width : (t + 1) * head_width])
    mixed[...] = low(jnp.transpose(jnp.concatenate(parts, axis=0)))


def attention(qkv, hot, bias, head_width):
    tokens = qkv[0].shape[0]
    heads = bias.shape[0]
    per = 128 // head_width
    groups = heads // per
    full = lambda g: (0, 0)
    pair = pl.BlockSpec((tokens, 128), lambda g: (0, g))
    return pl.pallas_call(
        partial(attention_kernel, head_width, head_width**-0.5),
        grid=(groups,),
        out_shape=(
            jax.ShapeDtypeStruct((tokens, heads * head_width), BF16),
            jax.ShapeDtypeStruct((heads, tokens, tokens), BF16),
        ),
        in_specs=[pair] * 5
        + [
            pl.BlockSpec(hot.shape, full),
            pl.BlockSpec((per,) + bias.shape[1:], lambda g: (g, 0, 0)),
        ],
        out_specs=[
            pair,
            pl.BlockSpec((per, tokens, tokens), lambda g: (g, 0, 0)),
        ],
        compiler_params=pltpu.CompilerParams(vmem_limit_bytes=48 << 20),
        name="attention",
    )(*qkv, hot, bias)


def attention_back_kernel(
    head_width, scale, groups, q, k, v, sq, sk, hot_ref, probs, mixed_grad, grad, sgrad, corner
):
    g = pl.program_id(0)
    keys = jnp.concatenate([k[...], sk[...]], axis=1)
    queries = jnp.concatenate([q[...], sq[...]], axis=1) * scale
    hot = hot_ref[...]
    value = v[...]
    outer = mixed_grad[...]
    key_total = value_total = None
    query_rows = [[], []]
    for t in range(128 // head_width):
        outer_t = outer * pair_mask(128, head_width, t)
        prob = probs[t]
        prob_wide = wide(prob)
        prob_grad = dot(value, outer_t, 1, 1)
        delta = jnp.sum(prob_wide * prob_grad, axis=0, keepdims=True)
        score_grad = low(prob_wide * (prob_grad - delta))
        value_part = dot(prob, outer_t)
        key_part = dot(score_grad, queries * pair_mask(256, head_width, t))
        key_total = key_part if t == 0 else key_total + key_part
        value_total = value_part if t == 0 else value_total + value_part
        query_t = dot(keys, score_grad, 0, 0)
        for half in range(2):
            start = half * 128 + t * head_width
            query_rows[half].append(query_t[start : start + head_width])
        feature_grad = dot(hot, score_grad, 0, 0)
        high = low(feature_grad)
        rest = low(feature_grad - wide(high))
        corner[t] = dot(high, hot) + dot(rest, hot)
    query_total = jnp.transpose(jnp.concatenate(query_rows[0] + query_rows[1], axis=0)) * scale

    def place(j):
        return pl.ds(pl.multiple_of(j * groups * 128 + g * 128, 128), 128)

    grad[:, place(0)] = low(query_total[:, :128])
    grad[:, place(1)] = low(key_total[:, :128])
    grad[:, place(2)] = low(value_total)
    sgrad[:, place(0)] = low(query_total[:, 128:])
    sgrad[:, place(1)] = low(key_total[:, 128:])


def attention_back(qkv, hot, probs, mixed_grad, head_width):
    tokens, own_width = qkv[0].shape
    heads = probs.shape[0]
    per = 128 // head_width
    groups = heads // per
    wide_hot = hot.shape[1]
    full = lambda g: (0, 0)
    pair = pl.BlockSpec((tokens, 128), lambda g: (0, g))
    return pl.pallas_call(
        partial(attention_back_kernel, head_width, head_width**-0.5, groups),
        grid=(groups,),
        out_shape=(
            jax.ShapeDtypeStruct((tokens, 3 * own_width), BF16),
            jax.ShapeDtypeStruct((tokens, 2 * own_width), BF16),
            jax.ShapeDtypeStruct((heads, wide_hot, wide_hot), F32),
        ),
        in_specs=[pair] * 5
        + [
            pl.BlockSpec(hot.shape, full),
            pl.BlockSpec((per, tokens, tokens), lambda g: (g, 0, 0)),
            pair,
        ],
        out_specs=[
            pl.BlockSpec((tokens, 3 * own_width), full),
            pl.BlockSpec((tokens, 2 * own_width), full),
            pl.BlockSpec((per, wide_hot, wide_hot), lambda g: (g, 0, 0)),
        ],
        compiler_params=pltpu.CompilerParams(vmem_limit_bytes=48 << 20),
        name="attention_back",
    )(*qkv, hot, probs, mixed_grad)


def norm_forward(residual, gain_row, bias_row):
    centre = residual - jnp.mean(residual, axis=-1, keepdims=True)
    inv_std = lax.rsqrt(jnp.mean(centre * centre, axis=-1, keepdims=True) + EPSILON)
    normed = centre * inv_std
    return normed * gain_row + bias_row, normed, inv_std


def norm_backward(grad_out, normed, inv_std, gain_row):
    scaled = grad_out * gain_row
    mean_one = jnp.mean(scaled, axis=-1, keepdims=True)
    mean_two = jnp.mean(scaled * normed, axis=-1, keepdims=True)
    grad_in = inv_std * (scaled - mean_one - normed * mean_two)
    return grad_in, jnp.sum(grad_out * normed, axis=0), jnp.sum(grad_out, axis=0)


def per_device(
    fsdp,
    activations,
    spatial,
    buckets,
    page_valid,
    qkv_w,
    out_w,
    up_w,
    down_w,
    spatial_w,
    tables,
    norm_gains,
    biases,
    cotangent,
):
    rows, width = activations.shape[2:]
    tokens = buckets.shape[3]
    heads = tables.shape[3]
    head_width = width // heads
    bins = (tables.shape[4] + 1) // 2
    own_heads = heads // 2
    own_width = width // 2
    shard_rows = qkv_w.shape[3]
    ff = up_w.shape[3]
    unit = ff // fsdp // 2
    own_ff = ff // 2
    rep = lax.axis_index("rep")
    y, c = rep // 2, rep % 2

    def columns(array, axis):
        return lax.dynamic_slice_in_dim(array, c * own_width, own_width, axis)

    params = jnp.concatenate([pick(norm_gains[0], y), pick(biases[0], y)])
    params = jnp.pad(params, ((0, 12), (0, -shard_rows % 128)))[None]
    up_part = pick(pick(up_w[0], y).reshape(shard_rows, fsdp, 2, unit), c, 2)
    up_part = up_part.reshape(1, shard_rows, own_ff)
    weights = (qkv_w, out_w, down_w, spatial_w)
    own = tokens // 2
    block = rows
    valid = page_valid[0] > 0

    page_buckets = pick(buckets, y)[:, 0].reshape(3, 4, block)
    order = [rep, y_of(rep), c_of(rep), y_of(c_of(rep))]
    page_buckets = jnp.concatenate([pick(page_buckets, i, 1) for i in order], axis=1)
    hot = (page_buckets[..., None] == jnp.arange(bins, dtype=jnp.int32)).astype(BF16)
    hot = jnp.transpose(hot, (1, 0, 2)).reshape(tokens, 3 * bins)
    left = lax.broadcasted_iota(jnp.int32, (bins, bins, 2 * bins - 1), 0)
    right = lax.broadcasted_iota(jnp.int32, (bins, bins, 2 * bins - 1), 1)
    slot = lax.broadcasted_iota(jnp.int32, (bins, bins, 2 * bins - 1), 2)
    offsets = (left - right + bins - 1 == slot).astype(F32)
    own_tables = lax.dynamic_slice_in_dim(pick(tables[0], y), c * own_heads, own_heads, 1)
    matrices = jnp.einsum("khr,uvr->hkuv", wide(own_tables), offsets, precision=HIGHEST)
    bias = jnp.einsum("hkuv,kq->hkuqv", matrices, jnp.eye(3, dtype=F32), precision=HIGHEST)
    bias = low(bias.reshape(own_heads, 3 * bins, 3 * bins))

    def core_sum(partial_sum):
        return partial_sum[:own] + wide(core_swap(low(partial_sum[own:])))

    def both_cores(value):
        return jnp.concatenate([value, core_swap(value)])

    def other_stream(value):
        sent = low(value)
        return wide(y_swap(jnp.concatenate([sent[block:], sent[:block]])))

    if fsdp == 8:
        flags = jnp.broadcast_to(wide(page_valid)[:, None], (8, 128))
        done = forward(
            fsdp,
            head_width,
            weights,
            up_part,
            params,
            activations,
            spatial,
            cotangent,
            hot,
            bias,
            flags,
        )
        gathered = done[:9]
        proj, probs, mixed, w_own, hidden_all, gate, active = done[9:16]
        normed_one, inv_one, normed_two, inv_two, layer_out = done[16:]
        inv_one, inv_two = inv_one[:, :1], inv_two[:, :1]
        qkv = [proj[j] for j in range(5)]
        layer_out = layer_out[:, None]
    else:
        gathered = gather_plain(weights, up_part, params, activations, spatial, cotangent, y, c)
    norms = gathered[3][0]
    gathered = [g.reshape(g.shape[0], -1, g.shape[3]) for g in gathered[:3] + gathered[4:6]] + [
        g.reshape(-1, width) for g in gathered[6:]
    ]
    w_qkv, w_spatial, (w_out,), (w_up,), (w_down,), x_all, s_all, cot = gathered
    norms = wide(jnp.transpose(norms[:, :4, :shard_rows], (1, 0, 2)).reshape(4, 1, width))
    gain_one, gain_two, bias_one, bias_two = [norms[i] for i in range(4)]
    if fsdp != 8:
        mine = lax.dynamic_slice(w_out, (c * own_width, 0), (own_width, own_width))
        give = lax.dynamic_slice(w_out, ((1 - c) * own_width, 0), (own_width, own_width))
        w_own = ordered(c, mine, core_swap(give), 1).reshape(own_width, width)
        x_own = wide(x_all[:own])
        qkv = [low(dot(x_all, w_qkv[j])) for j in range(3)]
        qkv += [low(dot(s_all, w_spatial[j])) for j in range(2)]
        mixed, probs = attention(qkv, hot, bias, head_width)
        branch = core_sum(dot(mixed, w_own))
        residual = x_own + (branch + other_stream(branch))
        hidden, normed_one, inv_one = norm_forward(residual, gain_one, bias_one)
        hidden_all = both_cores(low(hidden))
        gate = dot(hidden_all, w_up)
        active = low(jax.nn.gelu(gate, approximate=True))
        ffn = core_sum(dot(active, w_down))
        result, normed_two, inv_two = norm_forward(hidden + ffn, gain_two, bias_two)
        layer_out = low(jnp.where(valid, result, x_own))
        layer_out = ordered(y, layer_out[:block], y_swap(layer_out[block:]), 0)[:, None]

    upstream = jnp.where(valid, wide(cot), 0.0)
    back_two, gain_two_grad, bias_two_grad = norm_backward(upstream, normed_two, inv_two, gain_two)
    ffn_grad = both_cores(low(back_two))
    down_grad = low(dot(active, ffn_grad, 0, 0))
    active_grad = dot(ffn_grad, w_down, 1, 1)
    pull = jax.vjp(partial(jax.nn.gelu, approximate=True), gate)[1]
    gate_grad = low(pull(active_grad)[0])
    up_grad = low(dot(hidden_all, gate_grad, 0, 0))
    hidden_grad = back_two + core_sum(dot(gate_grad, w_up, 1, 1))
    back_one, gain_one_grad, bias_one_grad = norm_backward(
        hidden_grad, normed_one, inv_one, gain_one
    )
    branch_grad = both_cores(low(back_one + other_stream(back_one)))
    mixed_grad = low(dot(branch_grad, w_own, 1, 1))
    out_own = low(dot(mixed, branch_grad, 0, 0))
    out_kept = columns(out_own, 1)
    out_given = lax.dynamic_slice_in_dim(out_own, (1 - c) * own_width, own_width, 1)
    out_grad = ordered(c, out_kept, core_swap(out_given), 0).reshape(width, own_width)
    norm_grads = jnp.stack([gain_one_grad, gain_two_grad, bias_one_grad, bias_two_grad], 1)
    out_grad = jnp.concatenate([out_grad, jnp.pad(low(norm_grads), ((0, 0), (0, 124)))], axis=1)
    grad, sgrad, corner = attention_back(qkv, hot, probs, mixed_grad, head_width)
    qkv_grad = low(dot(x_all, grad, 0, 0))
    spatial_grad = low(dot(s_all, sgrad, 0, 0))
    back = sum(
        dot(grad[:, j * own_width : (j + 1) * own_width], w_qkv[j], 1, 1) for j in range(3)
    )
    in_own = back_one + core_sum(back)
    in_own = jnp.where(valid, in_own, wide(cot))
    in_far = wide(y_swap(low(in_own[block:])))
    in_grad = ordered(y, in_own[:block], in_far, 0)[:, None]

    corner = corner.reshape(own_heads, 3, bins, 3, bins)
    corner = jnp.stack([corner[:, k, :, k, :] for k in range(3)])
    table = jnp.einsum("khvu,uvr->khr", corner, offsets, precision=HIGHEST)
    flat = own_heads * (2 * bins - 1)
    table = jnp.pad(table.reshape(3, flat), ((0, 5), (0, -flat % 128)))

    grads = [
        g.reshape(fsdp, -1, g.shape[1])
        for g in (down_grad, up_grad, qkv_grad, spatial_grad, out_grad)
    ]
    shapes = (down_w.shape, up_w.shape, qkv_w.shape, spatial_w.shape, out_w.shape)
    if fsdp == 8:
        reduced = reduce(fsdp, grads, table)
        finished = finish(own_width, unit, reduced[:5], shapes)
    else:
        reduced = reduce_plain(grads, table)
        finished = finish_plain(y, c, fsdp, reduced[:5], shapes)
    down_grad, up_grad, qkv_grad, spatial_grad, out_grad = finished
    table = reduced[5][:, :3, :flat].reshape(4, 3, own_heads, -1)
    table = [ordered(c, table[2 * s], table[2 * s + 1], 1) for s in range(2)]
    table_grad = ordered(y, table[0], table[1], 0).reshape(tables.shape)
    norm_sum = wide(reduced[4][:, :, own_width : own_width + 4])
    norm_sum = jnp.transpose(norm_sum[0::2] + norm_sum[1::2], (0, 2, 1))
    norm_sum = ordered(y, norm_sum[0], norm_sum[1], 0)
    gain_grad, bias_grad = norm_sum[None, :, :2], norm_sum[None, :, 2:]
    return (
        layer_out,
        in_grad,
        qkv_grad,
        out_grad,
        up_grad,
        down_grad,
        spatial_grad,
        table_grad,
        gain_grad,
        bias_grad,
    )


def y_of(rep):
    return (rep + 2) % 4


def c_of(rep):
    return rep + 1 - 2 * (rep % 2)


def solution(mesh):
    weight = P(None, None, "fsdp", None)
    tokens = P(None, "fsdp", "rep", None)
    qkv = P(None, None, None, "fsdp", None)
    norm = P(None, None, None, "fsdp")
    return jax.shard_map(
        partial(per_device, mesh.shape["fsdp"]),
        mesh=mesh,
        in_specs=(
            tokens,
            tokens,
            weight,
            P("fsdp"),
            qkv,
            weight,
            weight,
            weight,
            P(None, "fsdp", None),
            P(),
            norm,
            norm,
            tokens,
        ),
        out_specs=(
            tokens,
            tokens,
            qkv,
            weight,
            weight,
            weight,
            P(None, "fsdp", None),
            P(),
            norm,
            norm,
        ),
        check_vma=False,
    )
```
